32 devices in a mesh: colour: 2 (over core), sub: 16 (over z, y, x).
Axes of the slice: x: 2, y: 2, z: 4, core: 2. Of those that a mesh axis runs over, the one named last changes fastest.
Arguments:
- rhs: float32 [3, 64, 256, 512], P(None, 'sub'), may hold values from -60 to 60
- diagonal: float32 [64, 256, 512], P('sub'), may hold values from 0.2 to 6
Outputs:
- solution: float32 [3, 64, 256, 512], P(None, 'sub', None, 'colour')
- residual: float32 [3, 64, 256, 512], P(None, 'sub', None, 'colour')
- norms: float32 [3], replicated
The draws below stay inside these ranges and needn't reach their ends.
All inputs are finite; a program needn't handle non-finite values.
Results may differ from the reference program's by a relative error of at most 0.0003.
Values sent between devices are 32-bit elements; how exact they have to be, the bound alone decides.
A program may use at most 128 MiB of HBM per device.

```python
import math
import jax
import jax.numpy as jnp
from jax import lax

CX = 4
NY = 256
NZ = 512
RIM = 1
SWEEPS = 8
NRHS = 3
NX = 64
N_SUB = 16


def draw_rhs(key, part):
    first = jax.random.fold_in(jax.random.fold_in(key, 17), 0)
    base = jax.random.normal(first, (NRHS, NX, NY, NZ), jnp.float32)
    ramp = 1.0 + 2.0 * jnp.arange(NX, dtype=jnp.float32) / (NX - 1)
    ramp = ramp[None, :, None, None]
    field = base * ramp
    return jnp.clip(field, -60.0, 60.0)


def level_of(rng, extent, shards, low, largest):
    gain = 1.0
    for axis_at, parts in shards:
        steps = jax.random.uniform(jax.random.fold_in(jax.random.fold_in(rng, 6), axis_at), (parts,), jnp.float32, low / len(shards), largest / len(shards))
        gain = gain * jnp.repeat(jnp.exp(steps), extent[axis_at] // parts).reshape((-1,) + (1,) * (len(extent) - 1 - axis_at))
    return gain


def setup_inputs(seed: int = 0) -> dict:
    seeds = jax.random.split(jax.random.key(seed), 3)
    return {
        "rhs": draw_rhs(jax.random.fold_in(seeds[2], 71), 0),
        "diagonal": jnp.clip(jnp.exp(math.log(6.0) - 3.4011974 * jax.random.uniform(seeds[1], (NX, NY, NZ), jnp.float32) ** level_of(seeds[1], (NX, NY, NZ), ((0, 16),), -0.2, 0.2)), 0.2, 6.0),
    }


OMEGA = 0.8

def neighbours(field):
    pads = ((0, 0),) * (field.ndim - 3) + ((1, 1), (1, 1), (1, 1))
    padded = jnp.pad(field, pads)
    beside = padded[..., 2:, 1:-1, 1:-1] + padded[..., :-2, 1:-1, 1:-1]
    beside = beside + padded[..., 1:-1, 2:, 1:-1] + padded[..., 1:-1, :-2, 1:-1]
    beside = beside + padded[..., 1:-1, 1:-1, 2:] + padded[..., 1:-1, 1:-1, :-2]
    return beside

def jacobi(resid, diag, mask):
    scale = OMEGA / (6.0 + diag)
    found = jnp.zeros_like(resid)
    for sweep in range(SWEEPS):
        found = (found + scale * (resid - (6.0 + diag) * found + neighbours(found))) * mask
    return found

def operate(field, diagonal):
    return (6.0 + diagonal) * field - neighbours(field)

def reference(rhs, diagonal):
    half = CX // 2
    span = half + 2 * RIM
    padded_diag = jnp.pad(diagonal, ((RIM, RIM), (0, 0), (0, 0)))
    layouts = []
    for colour in range(2):
        starts = jnp.arange(N_SUB, dtype=jnp.int32) * CX + colour * half
        index = (starts[:, None] + jnp.arange(span, dtype=jnp.int32)[None, :]).astype(jnp.int32)
        place = index - RIM
        mask = ((place >= 0) & (place < NX)).astype(jnp.float32)[:, :, None, None]
        layouts.append((index, mask, padded_diag[index]))

    def correction(resid, layout):
        index, mask, diag_regions = layout
        padded = jnp.pad(resid, ((RIM, RIM), (0, 0), (0, 0)))
        regions = padded[index] * mask
        found = jacobi(regions, diag_regions, mask)
        total = jnp.zeros_like(padded).at[index.reshape(-1)].add(found.reshape(-1, NY, NZ))
        return total[RIM:RIM + NX]

    def one_rhs(source):
        current = jnp.zeros_like(source)
        resid = source
        for colour in range(2):
            corr = correction(resid, layouts[colour])
            image = operate(corr, diagonal)
            alpha = jnp.sum(resid * corr) / jnp.sum(corr * image)
            current = current + alpha * corr
            resid = resid - alpha * image
        return (current, resid, jnp.sqrt(jnp.sum(resid * resid)))
    solution, residual, norms = lax.map(one_rhs, rhs)
    return (solution, residual, norms)
```

```python
import functools

import jax
import jax.numpy as jnp
from jax import lax
from jax.experimental import pallas as pl
from jax.experimental.pallas import tpu as pltpu
from jax.sharding import PartitionSpec as P

SWEEPS = 8
OMEGA = 0.8
ROWS = 8
LANES = 128
RIM = 8
PAD = 8
MESH = pl.DeviceIdType.MESH


def lane(t):
    return slice(t * LANES, (t + 1) * LANES)


def beside_lanes(at, row, t):
    zero = jnp.zeros_like(row[t])
    low = row[t - 1] if t > 0 else zero
    high = row[t + 1] if t + 1 < len(row) else zero
    left = pltpu.roll(jnp.where(at == LANES - 1, low, row[t]), 1, 1)
    right = pltpu.roll(jnp.where(at == 0, high, row[t]), LANES - 1, 1)
    return left + right


def kernel(
    count, rhs, diagonal, sol, res, norms, q, c0, c1, img, dg, sc, e, al, slots, mine,
    load_sem, q_send, q_recv, d_send, d_recv, c_send, c_recv, u_send, u_recv, r_send, r_recv,
    a_send, a_recv, o_local, o_send, o_recv,
):
    colour = lax.axis_index("colour")
    sub = lax.axis_index("sub")
    nrhs, cx, ny, nz = rhs.shape
    span = cx // 2 + 2
    tiles = nz // LANES
    own_rows = ny // 2
    rows = own_rows + RIM
    begin = pl.multiple_of(colour * (own_rows - RIM), ROWS)
    own = pl.multiple_of(colour * RIM, ROWS)
    everyone = 2 * count
    me = colour * count + sub
    has_left = sub > 0
    has_right = sub < count - 1
    left = (colour, sub - 1)
    right = (colour, sub + 1)
    partner = (1 - colour, sub)
    at = lax.broadcasted_iota(jnp.int32, (ROWS, LANES), 1)
    whole = pl.ds(PAD, rows)

    def hbm(t, plane=slice(None)):
        return (plane, pl.ds(begin, rows), lane(t))

    for t in range(tiles):
        pltpu.make_async_copy(
            diagonal.at[hbm(t)], dg.at[1 : cx + 1, t], load_sem.at[nrhs]
        ).start()
    for n in range(nrhs):
        for t in range(tiles):
            pltpu.make_async_copy(
                rhs.at[(n,) + hbm(t)], q.at[n, 1 : cx + 1, t], load_sem.at[n]
            ).start()

    barrier = pltpu.get_barrier_semaphore()

    def peer_of(i):
        other = lax.rem(me + i, everyone)
        return (other // count, lax.rem(other, count))

    def greet(i, carry):
        pl.semaphore_signal(barrier, inc=1, device_id=peer_of(i), device_id_type=MESH)
        return carry

    lax.fori_loop(1, everyone, greet, 0)

    zero = jnp.zeros((ROWS, LANES), jnp.float32)
    for t in range(tiles):
        for edge in (0, PAD + rows):
            for k in range(2):
                for p in range(span):
                    e[k, p, t, edge : edge + ROWS, :] = zero
            for n in range(nrhs):
                for p in range(cx + 2):
                    c0[n, p, t, edge : edge + ROWS, :] = zero
                    c1[n, p, t, edge : edge + ROWS, :] = zero

    def clear(ref, index, offset):
        def body(j, carry):
            r = pl.multiple_of(offset + j * ROWS, ROWS)
            for t in range(tiles):
                ref[index + (t, pl.ds(r, ROWS), slice(None))] = zero
            return carry

        lax.fori_loop(0, rows // ROWS, body, 0)

    @pl.when(jnp.logical_not(has_left))
    def _():
        clear(sc, (0,), 0)
        for n in range(nrhs):
            clear(q, (n, 0), 0)
            clear(c1, (n, 0), PAD)
            clear(c1, (n, 1), PAD)

    @pl.when(jnp.logical_not(has_right))
    def _():
        clear(sc, (cx + 1,), 0)
        for n in range(nrhs):
            clear(q, (n, cx + 1), 0)
            clear(c0, (n, cx), PAD)
            clear(c0, (n, cx + 1), PAD)

    pl.semaphore_wait(barrier, everyone - 1)

    def send(src, dst, send_sem, recv_sem, to):
        return pltpu.make_async_remote_copy(
            src_ref=src, dst_ref=dst, send_sem=send_sem, recv_sem=recv_sem,
            device_id=to, device_id_type=MESH,
        )

    def arrived(ref, sem):
        pltpu.make_async_copy(ref, ref, sem).wait()

    @pl.when(has_right)
    def _():
        for t in range(tiles):
            send(
                diagonal.at[hbm(t, cx - 1)], dg.at[0, t],
                q_send.at[nrhs], q_recv.at[nrhs], right,
            ).start()
        for n in range(nrhs):
            for t in range(tiles):
                send(
                    rhs.at[(n,) + hbm(t, cx - 1)], q.at[n, 0, t],
                    q_send.at[n], q_recv.at[n], right,
                ).start()

    @pl.when(has_left)
    def _():
        for t in range(tiles):
            send(diagonal.at[hbm(t, 0)], dg.at[cx + 1, t], d_send, d_recv, left).start()

    def scale_of(low, high):
        def body(j, carry):
            here = pl.ds(pl.multiple_of(j * ROWS, ROWS), ROWS)
            for p in range(low, high):
                for t in range(tiles):
                    full = 6.0 + dg[p, t, here, :]
                    dg[p, t, here, :] = full
                    sc[p, t, here, :] = OMEGA / full
            return carry

        lax.fori_loop(0, rows // ROWS, body, 0)

    arrived(dg.at[1 : cx + 1], load_sem.at[nrhs])
    scale_of(1, cx + 1)

    @pl.when(has_left)
    def _():
        arrived(dg.at[0], q_recv.at[nrhs])
        scale_of(0, 1)

    def solve(n, base, out):
        def first(j, carry):
            r = pl.multiple_of(j * ROWS, ROWS)
            here = pl.ds(r, ROWS)
            for p in range(span):
                for t in range(tiles):
                    e[0, p, t, pl.ds(r + PAD, ROWS), :] = (
                        sc[base + p, t, here, :] * q[n, base + p, t, here, :]
                    )
            return carry

        lax.fori_loop(0, rows // ROWS, first, 0, unroll=True)

        def sweep(src, write):
            def body(j, carry):
                r = pl.multiple_of(j * ROWS, ROWS)
                here = pl.ds(r, ROWS)
                planes = [
                    [e[src, p, t, pl.ds(r + PAD, ROWS), :] for t in range(tiles)]
                    for p in range(span)
                ]
                for p in range(span):
                    for t in range(tiles):
                        total = e[src, p, t, pl.ds(r + PAD - 1, ROWS), :]
                        total = total + e[src, p, t, pl.ds(r + PAD + 1, ROWS), :]
                        if p > 0:
                            total = total + planes[p - 1][t]
                        if p + 1 < span:
                            total = total + planes[p + 1][t]
                        total = total + beside_lanes(at, planes[p], t)
                        total = total + q[n, base + p, t, here, :]
                        value = (1.0 - OMEGA) * planes[p][t]
                        write(p, t, r, value + sc[base + p, t, here, :] * total)
                return carry

            lax.fori_loop(0, rows // ROWS, body, 0, unroll=True)

        def into(dst):
            def write(p, t, r, value):
                e[dst, p, t, pl.ds(r + PAD, ROWS), :] = value

            return write

        def write_out(p, t, r, value):
            out[n, base + p, t, pl.ds(r + PAD, ROWS), :] = value

        def two(s, carry):
            sweep(0, into(1))
            sweep(1, into(0))
            return carry

        lax.fori_loop(0, (SWEEPS - 2) // 2, two, 0)
        sweep(0, write_out)

    def image(n, c, extra):
        kinds = 5 if extra else 2

        def body(j, carry):
            r = pl.multiple_of(own + j * ROWS, ROWS)
            here = pl.ds(r, ROWS)
            sums = list(carry)
            planes = [
                [c[n, p, t, pl.ds(r + PAD, ROWS), :] for t in range(tiles)]
                for p in range(cx + 2)
            ]
            for p in range(1, cx + 1):
                for t in range(tiles):
                    total = c[n, p, t, pl.ds(r + PAD - 1, ROWS), :]
                    total = total + c[n, p, t, pl.ds(r + PAD + 1, ROWS), :]
                    total = total + planes[p - 1][t] + planes[p + 1][t]
                    total = total + beside_lanes(at, planes[p], t)
                    centre = planes[p][t]
                    value = dg[p, t, here, :] * centre - total
                    img[n, p - 1, t, here, :] = value
                    mine_q = q[n, p, t, here, :]
                    sums[0] = sums[0] + mine_q * centre
                    sums[1] = sums[1] + centre * value
                    if extra:
                        sums[2] = sums[2] + mine_q * mine_q
                        sums[3] = sums[3] + mine_q * value
                        sums[4] = sums[4] + value * value
            return tuple(sums)

        sums = lax.fori_loop(0, own_rows // ROWS, body, (zero,) * kinds, unroll=2)
        first = lax.broadcasted_iota(jnp.int32, (1, LANES), 1)
        row = jnp.zeros((1, LANES), jnp.float32)
        for i, value in enumerate(sums):
            row = jnp.where(first == i, jnp.sum(value), row)
        return row

    def share(k, n, row):
        mine[k, n] = row
        slots[k, n, me] = row

        def tell(i, carry):
            send(
                mine.at[k, n], slots.at[k, n, me], a_send.at[k, n], a_recv.at[k, n], peer_of(i)
            ).start()
            return carry

        lax.fori_loop(1, everyone, tell, 0)

    def totals(k, n):
        arrived(slots.at[k, n, pl.ds(0, everyone - 1)], a_recv.at[k, n])
        row = jnp.sum(slots[k, n], axis=0)
        first = lax.broadcasted_iota(jnp.int32, (1, LANES), 1)

        def pick(i):
            value = jnp.sum(jnp.where(first == i, row, 0.0), axis=1, keepdims=True)
            return jnp.broadcast_to(value, (ROWS, LANES))

        return pick

    edge_rows = pl.ds(PAD + own, own_rows)

    def c0_copies(n):
        return (
            send(
                c0.at[n, 0, :, whole], c0.at[n, cx, :, whole],
                c_send.at[0, n, 0], c_recv.at[0, n, 0], left,
            ),
            send(
                c0.at[n, 1, :, edge_rows], c0.at[n, cx + 1, :, edge_rows],
                c_send.at[0, n, 1], c_recv.at[0, n, 1], left,
            ),
        )

    def c1_copies(n):
        return (
            send(
                c1.at[n, cx + 1, :, whole], c1.at[n, 1, :, whole],
                c_send.at[1, n, 0], c_recv.at[1, n, 0], right,
            ),
            send(
                c1.at[n, cx, :, edge_rows], c1.at[n, 0, :, edge_rows],
                c_send.at[1, n, 1], c_recv.at[1, n, 1], right,
            ),
        )

    def q_copy(n):
        return send(q.at[n, 1], q.at[n, cx + 1], u_send.at[n], u_recv.at[n], left)

    rim_from = pl.multiple_of((1 - colour) * (own_rows - RIM) + colour * RIM, ROWS)
    rim_to = pl.multiple_of(colour * own_rows, ROWS)

    def rim_copy(n):
        return send(
            img.at[n, :, :, pl.ds(rim_from, RIM)], img.at[n, :, :, pl.ds(rim_to, RIM)],
            r_send.at[n], r_recv.at[n], partner,
        )

    def stage_a(n, carry):
        arrived(q.at[n, 1 : cx + 1], load_sem.at[n])

        @pl.when(has_left)
        def _():
            arrived(q.at[n, 0], q_recv.at[n])

        solve(n, 0, c0)

        @pl.when(has_left)
        def _():
            for copy in c0_copies(n):
                copy.start()

        return carry

    lax.fori_loop(0, nrhs, stage_a, 0)

    def stage_b(n, carry):
        @pl.when(n < nrhs)
        def _():
            @pl.when(has_right)
            def _():
                for copy in c0_copies(n):
                    copy.wait_recv()

            row = image(n, c0, False)
            rim_copy(n).start()
            share(0, n, row)

        @pl.when(n > 0)
        def _():
            m = n - 1
            pick = totals(0, m)
            alpha = pick(0) / pick(1)
            al[m] = alpha
            rim_copy(m).wait_recv()

            def body(j, carry):
                here = pl.ds(pl.multiple_of(j * ROWS, ROWS), ROWS)
                for p in range(cx):
                    for t in range(tiles):
                        value = q[m, p + 1, t, here, :] - alpha * img[m, p, t, here, :]
                        q[m, p + 1, t, here, :] = value
                return carry

            lax.fori_loop(0, rows // ROWS, body, 0)

            @pl.when(has_left)
            def _():
                q_copy(m).start()

        return carry

    lax.fori_loop(0, nrhs + 1, stage_b, 0)

    @pl.when(has_right)
    def _():
        arrived(dg.at[cx + 1], d_recv)
        scale_of(cx + 1, cx + 2)

    def stage_c(n, carry):
        @pl.when(has_right)
        def _():
            q_copy(n).wait_recv()

        solve(n, cx // 2, c1)

        @pl.when(has_right)
        def _():
            for copy in c1_copies(n):
                copy.start()

        return carry

    lax.fori_loop(0, nrhs, stage_c, 0)

    half = tiles // 2
    out_rows = pl.ds(pl.multiple_of(colour * own_rows, ROWS), own_rows)
    q_rows = pl.ds(own, own_rows)

    def out_copies(n):
        for t in range(half):
            for src, dst, r in ((c0, sol, edge_rows), (q, res, q_rows)):
                yield (
                    pltpu.make_async_copy(
                        src.at[n, 1 : cx + 1, colour * half + t, r],
                        dst.at[n, :, out_rows, lane(t)],
                        o_local.at[n],
                    ),
                    send(
                        src.at[n, 1 : cx + 1, (1 - colour) * half + t, r],
                        dst.at[n, :, out_rows, lane(t)],
                        o_send.at[n], o_recv.at[n], partner,
                    ),
                )

    def stage_d(n, carry):
        @pl.when(n < nrhs)
        def _():
            @pl.when(has_left)
            def _():
                for copy in c1_copies(n):
                    copy.wait_recv()

            rim_copy(n).wait_send()
            share(1, n, image(n, c1, True))

        @pl.when(n > 0)
        def _():
            m = n - 1

            @pl.when(has_left)
            def _():
                for copy in c0_copies(m):
                    copy.wait_send()
                q_copy(m).wait_send()

            pick = totals(1, m)
            alpha = pick(0) / pick(1)
            start = al[m]

            def body(j, carry):
                r = pl.multiple_of(own + j * ROWS, ROWS)
                here = pl.ds(r, ROWS)
                there = pl.ds(r + PAD, ROWS)
                for p in range(cx):
                    for t in range(tiles):
                        u = start * c0[m, p + 1, t, there, :] + alpha * c1[m, p + 1, t, there, :]
                        c0[m, p + 1, t, there, :] = u
                        value = q[m, p + 1, t, here, :] - alpha * img[m, p, t, here, :]
                        q[m, p + 1, t, here, :] = value
                return carry

            lax.fori_loop(0, own_rows // ROWS, body, 0)
            for local, remote in out_copies(m):
                local.start()
                remote.start()
            square = pick(2) - 2.0 * alpha * pick(3) + alpha * alpha * pick(4)
            norms[m] = jnp.sqrt(jnp.maximum(square, 0.0))

        return carry

    lax.fori_loop(0, nrhs + 1, stage_d, 0)

    @pl.when(has_right)
    def _():
        arrived(dg.at[0], q_send.at[nrhs])
        for n in range(nrhs):
            arrived(q.at[n, 0], q_send.at[n])
            for copy in c1_copies(n):
                copy.wait_send()

    @pl.when(has_left)
    def _():
        arrived(dg.at[cx + 1], d_send)

    for n in range(nrhs):
        for k in range(2):
            arrived(slots.at[k, n, pl.ds(0, everyone - 1)], a_send.at[k, n])
        for sem in (o_local, o_send, o_recv):
            arrived(c0.at[n, 1 : cx + 1, :, edge_rows], sem.at[n])


def shards(rhs, diagonal):
    count = lax.axis_size("sub")
    nrhs, cx, ny, nz = rhs.shape
    assert cx == 4 and SWEEPS % 2 == 0
    tiles = nz // LANES
    rows = ny // 2 + RIM
    padded = rows + 2 * PAD
    f32 = jnp.float32
    out = jax.ShapeDtypeStruct((nrhs, cx, ny, nz // 2), f32)
    dma = pltpu.SemaphoreType.DMA
    anywhere = pl.BlockSpec(memory_space=pl.ANY)
    sol, res, norms = pl.pallas_call(
        functools.partial(kernel, count),
        out_shape=(out, out, jax.ShapeDtypeStruct((nrhs, ROWS, LANES), f32)),
        in_specs=[anywhere, anywhere],
        out_specs=(anywhere, anywhere, pl.BlockSpec(memory_space=pltpu.VMEM)),
        scratch_shapes=[
            pltpu.VMEM((nrhs, cx + 2, tiles, rows, LANES), f32),
            pltpu.VMEM((nrhs, cx + 2, tiles, padded, LANES), f32),
            pltpu.VMEM((nrhs, cx + 2, tiles, padded, LANES), f32),
            pltpu.VMEM((nrhs, cx, tiles, rows, LANES), f32),
            pltpu.VMEM((cx + 2, tiles, rows, LANES), f32),
            pltpu.VMEM((cx + 2, tiles, rows, LANES), f32),
            pltpu.VMEM((2, cx // 2 + 2, tiles, padded, LANES), f32),
            pltpu.VMEM((nrhs, ROWS, LANES), f32),
            pltpu.VMEM((2, nrhs, 2 * count, 1, LANES), f32),
            pltpu.VMEM((2, nrhs, 1, LANES), f32),
            dma((nrhs + 1,)),
            dma((nrhs + 1,)), dma((nrhs + 1,)),
            dma, dma,
            dma((2, nrhs, 2)), dma((2, nrhs, 2)),
            dma((nrhs,)), dma((nrhs,)),
            dma((nrhs,)), dma((nrhs,)),
            dma((2, nrhs)), dma((2, nrhs)),
            dma((nrhs,)), dma((nrhs,)), dma((nrhs,)),
        ],
        compiler_params=pltpu.CompilerParams(
            collective_id=0, has_side_effects=True, vmem_limit_bytes=56 << 20
        ),
        name="schwarz",
    )(rhs, diagonal)
    return sol, res, norms[:, 0, 0]


def solution(mesh):
    placed = (P(None, "sub", None, None), P("sub", None, None))
    return jax.shard_map(
        shards,
        mesh=mesh,
        in_specs=placed,
        out_specs=(P(None, "sub", None, "colour"), P(None, "sub", None, "colour"), P()),
        check_vma=False,
    )
```

```python
import functools

import jax
import jax.numpy as jnp
from jax import lax
from jax.experimental import pallas as pl
from jax.experimental.pallas import tpu as pltpu
from jax.sharding import PartitionSpec as P

SWEEPS = 8
OMEGA = 0.8
ROWS = 8
LANES = 128
RIM = 8
PAD = 8
MESH = pl.DeviceIdType.MESH


def lane(t):
    return slice(t * LANES, (t + 1) * LANES)


def beside_lanes(at, row, t):
    zero = jnp.zeros_like(row[t])
    low = row[t - 1] if t > 0 else zero
    high = row[t + 1] if t + 1 < len(row) else zero
    left = pltpu.roll(jnp.where(at == LANES - 1, low, row[t]), 1, 1)
    right = pltpu.roll(jnp.where(at == 0, high, row[t]), LANES - 1, 1)
    return left + right


def kernel(
    count, rhs, diagonal, sol, res, norms, q, c0, c1, img, dg, sc, e, al, slots, mine,
    load_sem, q_send, q_recv, d_send, d_recv, c_send, c_recv, u_send, u_recv, r_send, r_recv,
    a_send, a_recv, o_send, o_recv,
):
    colour = lax.axis_index("colour")
    sub = lax.axis_index("sub")
    nrhs, cx, ny, nz = rhs.shape
    span = cx // 2 + 2
    tiles = nz // LANES
    own_rows = ny // 2
    rows = own_rows + RIM
    begin = pl.multiple_of(colour * (own_rows - RIM), ROWS)
    own = pl.multiple_of(colour * RIM, ROWS)
    everyone = 2 * count
    me = colour * count + sub
    has_left = sub > 0
    has_right = sub < count - 1
    left = (colour, sub - 1)
    right = (colour, sub + 1)
    partner = (1 - colour, sub)
    at = lax.broadcasted_iota(jnp.int32, (ROWS, LANES), 1)
    whole = pl.ds(PAD, rows)

    def hbm(t, plane=slice(None)):
        return (plane, pl.ds(begin, rows), lane(t))

    for t in range(tiles):
        pltpu.make_async_copy(
            diagonal.at[hbm(t)], dg.at[1 : cx + 1, t], load_sem.at[nrhs]
        ).start()
    for n in range(nrhs):
        for t in range(tiles):
            pltpu.make_async_copy(
                rhs.at[(n,) + hbm(t)], q.at[n, 1 : cx + 1, t], load_sem.at[n]
            ).start()

    barrier = pltpu.get_barrier_semaphore()

    def peer_of(i):
        other = lax.rem(me + i, everyone)
        return (other // count, lax.rem(other, count))

    def greet(i, carry):
        pl.semaphore_signal(barrier, inc=1, device_id=peer_of(i), device_id_type=MESH)
        return carry

    lax.fori_loop(1, everyone, greet, 0)

    zero = jnp.zeros((ROWS, LANES), jnp.float32)
    for t in range(tiles):
        for edge in (0, PAD + rows):
            for k in range(2):
                for p in range(span):
                    e[k, p, t, edge : edge + ROWS, :] = zero
            for n in range(nrhs):
                for p in range(cx + 2):
                    c0[n, p, t, edge : edge + ROWS, :] = zero
                    c1[n, p, t, edge : edge + ROWS, :] = zero

    def clear(ref, index, offset):
        def body(j, carry):
            r = pl.multiple_of(offset + j * ROWS, ROWS)
            for t in range(tiles):
                ref[index + (t, pl.ds(r, ROWS), slice(None))] = zero
            return carry

        lax.fori_loop(0, rows // ROWS, body, 0)

    @pl.when(jnp.logical_not(has_left))
    def _():
        clear(sc, (0,), 0)
        for n in range(nrhs):
            clear(q, (n, 0), 0)
            clear(c1, (n, 0), PAD)
            clear(c1, (n, 1), PAD)

    @pl.when(jnp.logical_not(has_right))
    def _():
        clear(sc, (cx + 1,), 0)
        for n in range(nrhs):
            clear(q, (n, cx + 1), 0)
            clear(c0, (n, cx), PAD)
            clear(c0, (n, cx + 1), PAD)

    with jax.named_scope("barrier"):
        pl.semaphore_wait(barrier, everyone - 1)

    def send(src, dst, send_sem, recv_sem, to):
        return pltpu.make_async_remote_copy(
            src_ref=src, dst_ref=dst, send_sem=send_sem, recv_sem=recv_sem,
            device_id=to, device_id_type=MESH,
        )

    def arrived(ref, sem):
        pltpu.make_async_copy(ref, ref, sem).wait()

    @pl.when(has_right)
    def _():
        for t in range(tiles):
            send(
                diagonal.at[hbm(t, cx - 1)], dg.at[0, t],
                q_send.at[nrhs], q_recv.at[nrhs], right,
            ).start()
        for n in range(nrhs):
            for t in range(tiles):
                send(
                    rhs.at[(n,) + hbm(t, cx - 1)], q.at[n, 0, t],
                    q_send.at[n], q_recv.at[n], right,
                ).start()

    def scale_of(low, high):
        def body(j, carry):
            here = pl.ds(pl.multiple_of(j * ROWS, ROWS), ROWS)
            for p in range(low, high):
                for t in range(tiles):
                    full = 6.0 + dg[p, t, here, :]
                    dg[p, t, here, :] = full
                    sc[p, t, here, :] = OMEGA / full
            return carry

        lax.fori_loop(0, rows // ROWS, body, 0)

    arrived(dg.at[1 : cx + 1], load_sem.at[nrhs])
    scale_of(1, cx + 1)

    @pl.when(has_left)
    def _():
        with jax.named_scope("d_wait"):
            arrived(dg.at[0], q_recv.at[nrhs])
            scale_of(0, 1)

    def solve(n, base, out):
        def first(j, carry):
            r = pl.multiple_of(j * ROWS, ROWS)
            here = pl.ds(r, ROWS)
            for p in range(span):
                for t in range(tiles):
                    e[0, p, t, pl.ds(r + PAD, ROWS), :] = (
                        sc[base + p, t, here, :] * q[n, base + p, t, here, :]
                    )
            return carry

        lax.fori_loop(0, rows // ROWS, first, 0)

        def sweep(src, write):
            def body(j, carry):
                r = pl.multiple_of(j * ROWS, ROWS)
                here = pl.ds(r, ROWS)
                planes = [
                    [e[src, p, t, pl.ds(r + PAD, ROWS), :] for t in range(tiles)]
                    for p in range(span)
                ]
                for p in range(span):
                    for t in range(tiles):
                        total = e[src, p, t, pl.ds(r + PAD - 1, ROWS), :]
                        total = total + e[src, p, t, pl.ds(r + PAD + 1, ROWS), :]
                        if p > 0:
                            total = total + planes[p - 1][t]
                        if p + 1 < span:
                            total = total + planes[p + 1][t]
                        total = total + beside_lanes(at, planes[p], t)
                        total = total + q[n, base + p, t, here, :]
                        value = (1.0 - OMEGA) * planes[p][t]
                        write(p, t, r, value + sc[base + p, t, here, :] * total)
                return carry

            lax.fori_loop(0, rows // ROWS, body, 0, unroll=True)

        def into(dst):
            def write(p, t, r, value):
                e[dst, p, t, pl.ds(r + PAD, ROWS), :] = value

            return write

        def write_out(p, t, r, value):
            out[n, base + p, t, pl.ds(r + PAD, ROWS), :] = value

        def two(s, carry):
            sweep(0, into(1))
            sweep(1, into(0))
            return carry

        lax.fori_loop(0, (SWEEPS - 2) // 2, two, 0)
        sweep(0, write_out)

    def image(n, c, low, high, sums, extra):
        def body(j, carry):
            r = pl.multiple_of(own + j * ROWS, ROWS)
            here = pl.ds(r, ROWS)
            sums = list(carry)
            planes = {
                p: [c[n, p, t, pl.ds(r + PAD, ROWS), :] for t in range(tiles)]
                for p in range(low - 1, high + 1)
            }
            for p in range(low, high):
                for t in range(tiles):
                    total = c[n, p, t, pl.ds(r + PAD - 1, ROWS), :]
                    total = total + c[n, p, t, pl.ds(r + PAD + 1, ROWS), :]
                    total = total + planes[p - 1][t] + planes[p + 1][t]
                    total = total + beside_lanes(at, planes[p], t)
                    centre = planes[p][t]
                    value = dg[p, t, here, :] * centre - total
                    img[n, p - 1, t, here, :] = value
                    mine_q = q[n, p, t, here, :]
                    sums[0] = sums[0] + mine_q * centre
                    sums[1] = sums[1] + centre * value
                    if extra:
                        sums[2] = sums[2] + mine_q * mine_q
                        sums[3] = sums[3] + mine_q * value
                        sums[4] = sums[4] + value * value
            return tuple(sums)

        return lax.fori_loop(0, own_rows // ROWS, body, sums, unroll=4)

    def row_of(sums):
        first = lax.broadcasted_iota(jnp.int32, (1, LANES), 1)
        row = jnp.zeros((1, LANES), jnp.float32)
        for i, value in enumerate(sums):
            row = jnp.where(first == i, jnp.sum(value), row)
        return row

    def share(k, n, row):
        mine[k, n] = row
        slots[k, n, me] = row

        def tell(i, carry):
            send(
                mine.at[k, n], slots.at[k, n, me], a_send.at[k, n], a_recv.at[k, n], peer_of(i)
            ).start()
            return carry

        lax.fori_loop(1, everyone, tell, 0)

    def totals(k, n):
        arrived(slots.at[k, n, pl.ds(0, everyone - 1)], a_recv.at[k, n])
        row = jnp.sum(slots[k, n], axis=0)
        first = lax.broadcasted_iota(jnp.int32, (1, LANES), 1)

        def pick(i):
            value = jnp.sum(jnp.where(first == i, row, 0.0), axis=1, keepdims=True)
            return jnp.broadcast_to(value, (ROWS, LANES))

        return pick

    edge_rows = pl.ds(PAD + own, own_rows)

    def c0_copies(n):
        return (
            send(
                c0.at[n, 0, :, whole], c0.at[n, cx, :, whole],
                c_send.at[0, n, 0], c_recv.at[0, n, 0], left,
            ),
            send(
                c0.at[n, 1, :, edge_rows], c0.at[n, cx + 1, :, edge_rows],
                c_send.at[0, n, 1], c_recv.at[0, n, 1], left,
            ),
        )

    def c1_copies(n):
        return (
            send(
                c1.at[n, cx + 1, :, whole], c1.at[n, 1, :, whole],
                c_send.at[1, n, 0], c_recv.at[1, n, 0], right,
            ),
            send(
                c1.at[n, cx, :, edge_rows], c1.at[n, 0, :, edge_rows],
                c_send.at[1, n, 1], c_recv.at[1, n, 1], right,
            ),
        )

    def q_copy(n):
        return send(q.at[n, 1], q.at[n, cx + 1], u_send.at[n], u_recv.at[n], left)

    rim_from = pl.multiple_of((1 - colour) * (own_rows - RIM) + colour * RIM, ROWS)
    rim_to = pl.multiple_of(colour * own_rows, ROWS)

    def rim_copy(n):
        return send(
            img.at[n, :, :, pl.ds(rim_from, RIM)], img.at[n, :, :, pl.ds(rim_to, RIM)],
            r_send.at[n], r_recv.at[n], partner,
        )

    def pipeline(solve_one, send_one, look_one, finish_one):
        def body(k, carry):
            @pl.when(k < nrhs)
            def _():
                solve_one(k)

            @pl.when((k >= 2) & (k < nrhs + 2))
            def _():
                look_one(k - 2)

            @pl.when((k >= 2) & (k < nrhs))
            def _():
                send_one(k)

            @pl.when(k >= 3)
            def _():
                finish_one(k - 3)

            return carry

        lax.fori_loop(0, nrhs + 3, body, 0)

    def first_sends(n, send_one):
        @pl.when(n == nrhs - 1)
        def _():
            for m in range(2):
                send_one(m)

    def solve_0(n):
        arrived(q.at[n, 1 : cx + 1], load_sem.at[n])

        @pl.when(has_left)
        def _():
            with jax.named_scope("q_wait"):
                arrived(q.at[n, 0], q_recv.at[n])

        @pl.when((n == nrhs - 1) & has_left)
        def _():
            for t in range(tiles):
                send(diagonal.at[hbm(t, 0)], dg.at[cx + 1, t], d_send, d_recv, left).start()

        first_sends(n, send_0)
        with jax.named_scope("solve_0"):
            solve(n, 0, c0)

    def send_0(n):
        @pl.when(has_left)
        def _():
            for copy in c0_copies(n):
                copy.start()

    def look_0(n):
        with jax.named_scope("image_0"):
            sums = image(n, c0, 1, cx - 1, (zero,) * 2, False)

        @pl.when(has_right)
        def _():
            with jax.named_scope("c0_wait"):
                for copy in c0_copies(n):
                    copy.wait_recv()

        with jax.named_scope("image_0"):
            sums = image(n, c0, cx - 1, cx + 1, sums, False)
            row = row_of(sums)
            rim_copy(n).start()
            share(0, n, row)

    def finish_0(m):
        with jax.named_scope("total_0"):
            pick = totals(0, m)
            alpha = pick(0) / pick(1)
            al[m] = alpha
        with jax.named_scope("rim_wait"):
            rim_copy(m).wait_recv()

        def body(j, carry):
            here = pl.ds(pl.multiple_of(j * ROWS, ROWS), ROWS)
            for p in range(cx):
                for t in range(tiles):
                    value = q[m, p + 1, t, here, :] - alpha * img[m, p, t, here, :]
                    q[m, p + 1, t, here, :] = value
            return carry

        with jax.named_scope("update_0"):
            lax.fori_loop(0, rows // ROWS, body, 0)

        @pl.when(has_left)
        def _():
            q_copy(m).start()

    pipeline(solve_0, send_0, look_0, finish_0)

    @pl.when(has_right)
    def _():
        arrived(dg.at[cx + 1], d_recv)
        scale_of(cx + 1, cx + 2)

    def solve_1(n):
        @pl.when(has_right)
        def _():
            with jax.named_scope("q1_wait"):
                q_copy(n).wait_recv()

        first_sends(n, send_1)
        with jax.named_scope("solve_1"):
            solve(n, cx // 2, c1)

    def send_1(n):
        @pl.when(has_right)
        def _():
            for copy in c1_copies(n):
                copy.start()

    half = tiles // 2
    out_rows = pl.ds(pl.multiple_of(colour * own_rows, ROWS), own_rows)
    q_rows = pl.ds(own, own_rows)

    def out_copies(n):
        for t in range(half):
            for src, dst, r in ((c0, sol, edge_rows), (q, res, q_rows)):
                yield send(
                    src.at[n, 1 : cx + 1, (1 - colour) * half + t, r],
                    dst.at[n, :, out_rows, lane(t)],
                    o_send.at[n], o_recv.at[n], partner,
                )

    def look_1(n):
        rim_copy(n).wait_send()
        with jax.named_scope("image_1"):
            sums = image(n, c1, 3, cx + 1, (zero,) * 5, True)

        @pl.when(has_left)
        def _():
            with jax.named_scope("c1_wait"):
                for copy in c1_copies(n):
                    copy.wait_recv()

        with jax.named_scope("image_1"):
            sums = image(n, c1, 1, 3, sums, True)
            share(1, n, row_of(sums))

    def finish_1(m):
        @pl.when(has_left)
        def _():
            for copy in c0_copies(m):
                copy.wait_send()
            q_copy(m).wait_send()

        with jax.named_scope("total_1"):
            pick = totals(1, m)
            alpha = pick(0) / pick(1)
            start = al[m]

        def body(j, carry):
            r = pl.multiple_of(own + j * ROWS, ROWS)
            here = pl.ds(r, ROWS)
            there = pl.ds(r + PAD, ROWS)
            out = pl.ds(pl.multiple_of(colour * own_rows + j * ROWS, ROWS), ROWS)
            for p in range(cx):
                for i in range(half):
                    for side in (colour, 1 - colour):
                        t = side * half + i
                        u = start * c0[m, p + 1, t, there, :]
                        u = u + alpha * c1[m, p + 1, t, there, :]
                        value = q[m, p + 1, t, here, :] - alpha * img[m, p, t, here, :]
                        if side is colour:
                            sol[m, p, out, lane(i)] = u
                            res[m, p, out, lane(i)] = value
                        else:
                            c0[m, p + 1, t, there, :] = u
                            q[m, p + 1, t, here, :] = value
            return carry

        with jax.named_scope("finish"):
            lax.fori_loop(0, own_rows // ROWS, body, 0)
        for copy in out_copies(m):
            copy.start()
        square = pick(2) - 2.0 * alpha * pick(3) + alpha * alpha * pick(4)
        norms[m] = jnp.max(jnp.sqrt(jnp.maximum(square, 0.0)))

    pipeline(solve_1, send_1, look_1, finish_1)

    with jax.named_scope("drain"):
        @pl.when(has_right)
        def _():
            arrived(dg.at[0], q_send.at[nrhs])
            for n in range(nrhs):
                arrived(q.at[n, 0], q_send.at[n])
                for copy in c1_copies(n):
                    copy.wait_send()

        @pl.when(has_left)
        def _():
            arrived(dg.at[cx + 1], d_send)

        for n in range(nrhs):
            for k in range(2):
                arrived(slots.at[k, n, pl.ds(0, everyone - 1)], a_send.at[k, n])
            for sem in (o_send, o_recv):
                arrived(c0.at[n, 1 : cx + 1, :, edge_rows], sem.at[n])


def shards(rhs, diagonal):
    count = lax.axis_size("sub")
    nrhs, cx, ny, nz = rhs.shape
    assert cx == 4 and SWEEPS % 2 == 0
    tiles = nz // LANES
    rows = ny // 2 + RIM
    padded = rows + 2 * PAD
    f32 = jnp.float32
    out = jax.ShapeDtypeStruct((nrhs, cx, ny, nz // 2), f32)
    dma = pltpu.SemaphoreType.DMA
    remote = pl.BlockSpec(memory_space=pltpu.HBM)
    near = pl.BlockSpec(memory_space=pltpu.VMEM)
    sol, res, norms = pl.pallas_call(
        functools.partial(kernel, count),
        out_shape=(out, out, jax.ShapeDtypeStruct((nrhs,), f32)),
        in_specs=[remote, remote],
        out_specs=(near, near, pl.BlockSpec(memory_space=pltpu.SMEM)),
        scratch_shapes=[
            pltpu.VMEM((nrhs, cx + 2, tiles, rows, LANES), f32),
            pltpu.VMEM((nrhs, cx + 2, tiles, padded, LANES), f32),
            pltpu.VMEM((nrhs, cx + 2, tiles, padded, LANES), f32),
            pltpu.VMEM((nrhs, cx, tiles, rows, LANES), f32),
            pltpu.VMEM((cx + 2, tiles, rows, LANES), f32),
            pltpu.VMEM((cx + 2, tiles, rows, LANES), f32),
            pltpu.VMEM((2, cx // 2 + 2, tiles, padded, LANES), f32),
            pltpu.VMEM((nrhs, ROWS, LANES), f32),
            pltpu.VMEM((2, nrhs, 2 * count, 1, LANES), f32),
            pltpu.VMEM((2, nrhs, 1, LANES), f32),
            dma((nrhs + 1,)),
            dma((nrhs + 1,)), dma((nrhs + 1,)),
            dma, dma,
            dma((2, nrhs, 2)), dma((2, nrhs, 2)),
            dma((nrhs,)), dma((nrhs,)),
            dma((nrhs,)), dma((nrhs,)),
            dma((2, nrhs)), dma((2, nrhs)),
            dma((nrhs,)), dma((nrhs,)),
        ],
        compiler_params=pltpu.CompilerParams(
            collective_id=0, has_side_effects=True, vmem_limit_bytes=44 << 20
        ),
        name="schwarz",
    )(
        pltpu.with_memory_space_constraint(rhs, pltpu.HBM),
        pltpu.with_memory_space_constraint(diagonal, pltpu.HBM),
    )
    return sol, res, norms


def solution(mesh):
    placed = (P(None, "sub", None, None), P("sub", None, None))
    return jax.shard_map(
        shards,
        mesh=mesh,
        in_specs=placed,
        out_specs=(P(None, "sub", None, "colour"), P(None, "sub", None, "colour"), P()),
        check_vma=False,
    )
```

```python
import functools

import jax
import jax.numpy as jnp
from jax import lax
from jax.experimental import pallas as pl
from jax.experimental.pallas import tpu as pltpu
from jax.sharding import PartitionSpec as P

SWEEPS = 8
OMEGA = 0.8
ROWS = 8
LANES = 128
RIM = 8
PAD = 8
MESH = pl.DeviceIdType.MESH


def lane(t):
    return slice(t * LANES, (t + 1) * LANES)


def beside_lanes(at, row, t):
    zero = jnp.zeros_like(row[t])
    low = row[t - 1] if t > 0 else zero
    high = row[t + 1] if t + 1 < len(row) else zero
    left = pltpu.roll(jnp.where(at == LANES - 1, low, row[t]), 1, 1)
    right = pltpu.roll(jnp.where(at == 0, high, row[t]), LANES - 1, 1)
    return left + right


def kernel(
    count, rhs, diagonal, sol, res, norms, q, c0, c1, img, dg, sc, e, al, slots, mine,
    x_c0, x_q, x_c1, x_img, norm_row,
    load_sem, q_send, q_recv, d_send, d_recv, c_send, c_recv, u_send, u_recv, r_send, r_recv,
    a_send, a_recv, f_send, f_recv, x_send, x_recv,
):
    colour = lax.axis_index("colour")
    sub = lax.axis_index("sub")
    nrhs, cx, ny, nz = rhs.shape
    span = cx // 2 + 2
    tiles = nz // LANES
    own_rows = ny // 2
    rows = own_rows + RIM
    begin = pl.multiple_of(colour * (own_rows - RIM), ROWS)
    own = pl.multiple_of(colour * RIM, ROWS)
    everyone = 2 * count
    me = colour * count + sub
    has_left = sub > 0
    has_right = sub < count - 1
    left = (colour, sub - 1)
    right = (colour, sub + 1)
    partner = (1 - colour, sub)
    at = lax.broadcasted_iota(jnp.int32, (ROWS, LANES), 1)
    whole = pl.ds(PAD, rows)

    core_rows = pl.ds(pl.multiple_of(colour * own_rows, ROWS), own_rows)
    q_rows = pl.ds(own, own_rows)
    edge_rows = pl.ds(PAD + own, own_rows)

    def hbm(t):
        return (slice(None), pl.ds(begin, rows), lane(t))

    barrier = pltpu.get_barrier_semaphore()

    def every_peer(act):
        for other, first in ((colour, 1), (1 - colour, 0)):

            def body(i, carry):
                act((other, lax.rem(sub + i, count)))
                return carry

            lax.fori_loop(first, count, body, 0, unroll=3 if first else 4)

    every_peer(
        lambda to: pl.semaphore_signal(barrier, inc=1, device_id=to, device_id_type=MESH)
    )

    for t in range(tiles):
        pltpu.make_async_copy(
            diagonal.at[hbm(t)], dg.at[1 : cx + 1, t], load_sem.at[nrhs]
        ).start()
    for n in range(nrhs):
        for t in range(tiles):
            pltpu.make_async_copy(
                rhs.at[(n,) + hbm(t)], q.at[n, 1 : cx + 1, t], load_sem.at[n]
            ).start()

    zero = jnp.zeros((ROWS, LANES), jnp.float32)
    for t in range(tiles):
        for edge in (0, PAD + rows):
            for k in range(2):
                for p in range(span):
                    e[k, p, t, edge : edge + ROWS, :] = zero
            for n in range(nrhs):
                for p in range(cx + 2):
                    c0[n, p, t, edge : edge + ROWS, :] = zero
                    c1[n, p, t, edge : edge + ROWS, :] = zero

    def clear(ref, index, offset):
        def body(j, carry):
            r = pl.multiple_of(offset + j * ROWS, ROWS)
            for t in range(tiles):
                ref[index + (t, pl.ds(r, ROWS), slice(None))] = zero
            return carry

        lax.fori_loop(0, rows // ROWS, body, 0)

    @pl.when(jnp.logical_not(has_left))
    def _():
        clear(sc, (0,), 0)
        for n in range(nrhs):
            clear(q, (n, 0), 0)
            clear(c1, (n, 0), PAD)
            clear(c1, (n, 1), PAD)

    @pl.when(jnp.logical_not(has_right))
    def _():
        clear(sc, (cx + 1,), 0)
        for n in range(nrhs):
            clear(q, (n, cx + 1), 0)
            clear(c0, (n, cx), PAD)
            clear(c0, (n, cx + 1), PAD)

    with jax.named_scope("barrier"):
        pl.semaphore_wait(barrier, everyone - 1)

    def send(src, dst, send_sem, recv_sem, to):
        return pltpu.make_async_remote_copy(
            src_ref=src, dst_ref=dst, send_sem=send_sem, recv_sem=recv_sem,
            device_id=to, device_id_type=MESH,
        )

    def arrived(ref, sem):
        pltpu.make_async_copy(ref, ref, sem).wait()

    @pl.when(has_right)
    def _():
        for t in range(tiles):
            send(
                diagonal.at[cx - 1, core_rows, lane(t)], dg.at[0, t, q_rows],
                q_send.at[nrhs], q_recv.at[nrhs], right,
            ).start()
        for n in range(nrhs):
            for t in range(tiles):
                send(
                    rhs.at[n, cx - 1, core_rows, lane(t)], q.at[n, 0, t, q_rows],
                    q_send.at[n], q_recv.at[n], right,
                ).start()

    rim_from = (1 - colour) * (own_rows - RIM) + colour * RIM
    rim_to = colour * own_rows

    def rim_copy(ref, pad, send_sem, recv_sem):
        return send(
            ref.at[..., pl.ds(pl.multiple_of(rim_from + pad, ROWS), RIM), :],
            ref.at[..., pl.ds(pl.multiple_of(rim_to + pad, ROWS), RIM), :],
            send_sem, recv_sem, partner,
        )

    def img_rim(n):
        return rim_copy(img.at[n], 0, r_send.at[n], r_recv.at[n])

    def q_rim(n):
        return rim_copy(q.at[n, 0], 0, f_send.at[2 + n], f_recv.at[2 + n])

    def q1_rim(n):
        k = 2 + nrhs + n
        return rim_copy(q.at[n, cx + 1], 0, f_send.at[k], f_recv.at[k])

    def c0_rim(n):
        k = 2 + 2 * nrhs + n
        return rim_copy(c0.at[n, cx], PAD, f_send.at[k], f_recv.at[k])

    half = tiles // 2
    away = pl.ds((1 - colour) * half, half)

    def cross(k, n):
        src, dst = (
            (c0.at[n, 1 : cx + 1, away, edge_rows], x_c0.at[n]),
            (q.at[n, 1 : cx + 1, away, q_rows], x_q.at[n]),
            (c1.at[n, 2 : cx + 1, away, edge_rows], x_c1.at[n, 1:cx]),
            (c1.at[n, 1:2, away, edge_rows], x_c1.at[n, 0:1]),
            (img.at[n, 2:cx, away, q_rows], x_img.at[n, 2:cx]),
            (img.at[n, 0:2, away, q_rows], x_img.at[n, 0:2]),
        )[k]
        return send(src, dst, x_send.at[n, k], x_recv.at[n, k], partner)

    def scale_of(low, high):
        def body(j, carry):
            here = pl.ds(pl.multiple_of(j * ROWS, ROWS), ROWS)
            for p in range(low, high):
                for t in range(tiles):
                    full = 6.0 + dg[p, t, here, :]
                    dg[p, t, here, :] = full
                    sc[p, t, here, :] = OMEGA / full
            return carry

        lax.fori_loop(0, rows // ROWS, body, 0)

    arrived(dg.at[1 : cx + 1], load_sem.at[nrhs])
    scale_of(1, cx + 1)

    @pl.when(has_left)
    def _():
        with jax.named_scope("d_wait"):
            arrived(dg.at[0, :, q_rows], q_recv.at[nrhs])
            copy = rim_copy(dg.at[0], 0, f_send.at[0], f_recv.at[0])
            copy.start()
            copy.wait()
            scale_of(0, 1)

    def solve(n, base, out):
        def first(j, carry):
            r = pl.multiple_of(j * ROWS, ROWS)
            here = pl.ds(r, ROWS)
            for p in range(span):
                for t in range(tiles):
                    e[0, p, t, pl.ds(r + PAD, ROWS), :] = (
                        sc[base + p, t, here, :] * q[n, base + p, t, here, :]
                    )
            return carry

        lax.fori_loop(0, rows // ROWS, first, 0)

        def sweep(src, write):
            def body(j, carry):
                r = pl.multiple_of(j * ROWS, ROWS)
                here = pl.ds(r, ROWS)
                planes = [
                    [e[src, p, t, pl.ds(r + PAD, ROWS), :] for t in range(tiles)]
                    for p in range(span)
                ]
                for p in range(span):
                    for t in range(tiles):
                        total = e[src, p, t, pl.ds(r + PAD - 1, ROWS), :]
                        total = total + e[src, p, t, pl.ds(r + PAD + 1, ROWS), :]
                        if p > 0:
                            total = total + planes[p - 1][t]
                        if p + 1 < span:
                            total = total + planes[p + 1][t]
                        total = total + beside_lanes(at, planes[p], t)
                        total = total + q[n, base + p, t, here, :]
                        value = (1.0 - OMEGA) * planes[p][t]
                        write(p, t, r, value + sc[base + p, t, here, :] * total)
                return carry

            lax.fori_loop(0, rows // ROWS, body, 0, unroll=True)

        def into(dst):
            def write(p, t, r, value):
                e[dst, p, t, pl.ds(r + PAD, ROWS), :] = value

            return write

        def write_out(p, t, r, value):
            out[n, base + p, t, pl.ds(r + PAD, ROWS), :] = value

        def two(s, carry):
            sweep(0, into(1))
            sweep(1, into(0))
            return carry

        lax.fori_loop(0, (SWEEPS - 2) // 2, two, 0)
        sweep(0, write_out)

    def image(n, c, low, high, sums, extra):
        def body(j, carry):
            r = pl.multiple_of(own + j * ROWS, ROWS)
            here = pl.ds(r, ROWS)
            sums = list(carry)
            planes = {
                p: [c[n, p, t, pl.ds(r + PAD, ROWS), :] for t in range(tiles)]
                for p in range(low - 1, high + 1)
            }
            for p in range(low, high):
                for t in range(tiles):
                    total = c[n, p, t, pl.ds(r + PAD - 1, ROWS), :]
                    total = total + c[n, p, t, pl.ds(r + PAD + 1, ROWS), :]
                    total = total + planes[p - 1][t] + planes[p + 1][t]
                    total = total + beside_lanes(at, planes[p], t)
                    centre = planes[p][t]
                    value = dg[p, t, here, :] * centre - total
                    img[n, p - 1, t, here, :] = value
                    mine_q = q[n, p, t, here, :]
                    sums[0] = sums[0] + mine_q * centre
                    sums[1] = sums[1] + centre * value
                    if extra:
                        sums[2] = sums[2] + mine_q * value
                        sums[3] = sums[3] + value * value
            return tuple(sums)

        return lax.fori_loop(0, own_rows // ROWS, body, sums, unroll=4)

    def row_of(sums):
        first = lax.broadcasted_iota(jnp.int32, (1, LANES), 1)
        row = jnp.zeros((1, LANES), jnp.float32)
        for i, value in enumerate(sums):
            row = jnp.where(first == i, jnp.sum(value), row)
        return row

    def squares(n, cross_sum, square_sum):
        square = jnp.sum(square_sum)
        fit = jnp.sum(cross_sum) / jnp.where(square > 0.0, square, 1.0)

        def body(j, carry):
            here = pl.ds(pl.multiple_of(own + j * ROWS, ROWS), ROWS)
            low, mixed = list(carry[0]), list(carry[1])
            for p in range(cx):
                for t in range(tiles):
                    value = img[n, p, t, here, :]
                    rest = q[n, p + 1, t, here, :] - fit * value
                    low[p] = low[p] + rest * rest
                    mixed[p] = mixed[p] + rest * value
            return tuple(low), tuple(mixed)

        low, mixed = lax.fori_loop(
            0, own_rows // ROWS, body, ((zero,) * cx, (zero,) * cx), unroll=2
        )
        first = lax.broadcasted_iota(jnp.int32, (1, LANES), 1)
        row = jnp.zeros((1, LANES), jnp.float32)
        for i, value in enumerate((fit, jnp.sum(sum(low)), jnp.sum(sum(mixed)), square)):
            row = jnp.where(first == i, value, row)
        return row

    def norm_of(n, alpha):
        arrived(slots.at[2, n, pl.ds(0, everyone - 1)], a_recv.at[2, n])
        rows_of = slots[2, n]
        first = lax.broadcasted_iota(jnp.int32, rows_of.shape, 2)
        fit, low, mixed, square = (
            jnp.sum(jnp.where(first == i, rows_of, 0.0), axis=2, keepdims=True) for i in range(4)
        )
        gap = alpha[0:1, 0:1][None] - fit
        total = jnp.sum(low + gap * (gap * square - 2.0 * mixed), axis=0)
        return jnp.sqrt(jnp.maximum(jnp.broadcast_to(total, (1, LANES)), 0.0))

    def share(k, n, row):
        mine[k, n] = row
        slots[k, n, me] = row

        every_peer(
            lambda to: send(
                mine.at[k, n], slots.at[k, n, me], a_send.at[k, n], a_recv.at[k, n], to
            ).start()
        )

    def totals(k, n):
        arrived(slots.at[k, n, pl.ds(0, everyone - 1)], a_recv.at[k, n])
        row = jnp.sum(slots[k, n], axis=0)
        first = lax.broadcasted_iota(jnp.int32, (1, LANES), 1)

        def pick(i):
            value = jnp.sum(jnp.where(first == i, row, 0.0), axis=1, keepdims=True)
            return jnp.broadcast_to(value, (ROWS, LANES))

        return pick

    def c0_copies(n):
        return (
            send(
                c0.at[n, 0, :, edge_rows], c0.at[n, cx, :, edge_rows],
                c_send.at[0, n, 0], c_recv.at[0, n, 0], left,
            ),
            send(
                c0.at[n, 1, :, edge_rows], c0.at[n, cx + 1, :, edge_rows],
                c_send.at[0, n, 1], c_recv.at[0, n, 1], left,
            ),
        )

    def c1_copies(n):
        return (
            send(
                c1.at[n, cx + 1, :, whole], c1.at[n, 1, :, whole],
                c_send.at[1, n, 0], c_recv.at[1, n, 0], right,
            ),
            send(
                c1.at[n, cx, :, edge_rows], c1.at[n, 0, :, edge_rows],
                c_send.at[1, n, 1], c_recv.at[1, n, 1], right,
            ),
        )

    def q_copy(n):
        return send(
            q.at[n, 1, :, q_rows], q.at[n, cx + 1, :, q_rows], u_send.at[n], u_recv.at[n], left
        )

    def pipeline(solve_one, send_one, look_one, finish_one):
        def body(k, carry):
            @pl.when(k < nrhs)
            def _():
                solve_one(k)

            @pl.when((k >= 2) & (k < nrhs + 2))
            def _():
                look_one(k - 2)

            @pl.when((k >= 2) & (k < nrhs))
            def _():
                send_one(k)

            @pl.when(k >= 3)
            def _():
                finish_one(k - 3)

            return carry

        lax.fori_loop(0, nrhs + 3, body, 0)

    def q_here():
        for m in range(1, nrhs):
            arrived(q.at[m, 0, :, q_rows], q_recv.at[m])

    def solve_0(n):
        arrived(q.at[n, 1 : cx + 1], load_sem.at[n])

        @pl.when(n == 1)
        def _():
            with jax.named_scope("gate_0"):

                @pl.when(has_right)
                def _():
                    for m in range(nrhs):
                        arrived(q.at[m, 0, :, q_rows], q_send.at[m])

                @pl.when(jnp.logical_not(has_right))
                def _():
                    q_here()

                @pl.when(has_left)
                def _():
                    for t in range(tiles):
                        send(
                            diagonal.at[0, core_rows, lane(t)], dg.at[cx + 1, t, q_rows],
                            d_send, d_recv, left,
                        ).start()

                send_0(0)

                @pl.when(has_right & has_left)
                def _():
                    q_here()

                @pl.when(has_left)
                def _():
                    for m in range(1, nrhs):
                        q_rim(m).start()

        @pl.when(has_left)
        def _():
            with jax.named_scope("q_wait"):

                @pl.when(n == 0)
                def _():
                    arrived(q.at[0, 0, :, q_rows], q_recv.at[0])
                    q_rim(0).start()

                q_rim(n).wait_recv()

        with jax.named_scope("solve_0"):
            solve(n, 0, c0)

        @pl.when(n == 1)
        def _():
            send_0(1)

    def send_0(n):
        @pl.when(has_left)
        def _():
            for copy in c0_copies(n):
                copy.start()

    def look_0(n):
        with jax.named_scope("image_0"):
            sums = image(n, c0, 1, cx - 1, (zero,) * 2, False)

        @pl.when(has_right)
        def _():
            with jax.named_scope("c0_wait"):
                for copy in c0_copies(n):
                    copy.wait_recv()
                c0_rim(n).start()
                c0_rim(n).wait_recv()

        with jax.named_scope("image_0"):
            sums = image(n, c0, cx - 1, cx + 1, sums, False)
            share(0, n, row_of(sums))
            img_rim(n).start()
            cross(0, n).start()

    def finish_0(m):
        with jax.named_scope("total_0"):
            pick = totals(0, m)
            alpha = pick(0) / pick(1)
            al[m] = alpha
        with jax.named_scope("rim_wait"):
            img_rim(m).wait_recv()

        def body(j, carry):
            here = pl.ds(pl.multiple_of(j * ROWS, ROWS), ROWS)
            for p in range(cx):
                for t in range(tiles):
                    value = q[m, p + 1, t, here, :] - alpha * img[m, p, t, here, :]
                    q[m, p + 1, t, here, :] = value
            return carry

        with jax.named_scope("update_0"):
            lax.fori_loop(0, rows // ROWS, body, 0)

        @pl.when(has_left)
        def _():
            q_copy(m).start()

        cross(1, m).start()

    pipeline(solve_0, send_0, look_0, finish_0)

    @pl.when(has_right)
    def _():
        arrived(dg.at[cx + 1, :, q_rows], d_recv)
        copy = rim_copy(dg.at[cx + 1], 0, f_send.at[1], f_recv.at[1])
        copy.start()
        copy.wait()
        scale_of(cx + 1, cx + 2)

    def solve_1(n):
        @pl.when(has_right)
        def _():
            with jax.named_scope("q1_wait"):
                @pl.when(n == 0)
                def _():
                    q_copy(0).wait_recv()
                    q1_rim(0).start()

                @pl.when(n == 1)
                def _():
                    for m in range(1, nrhs):
                        q_copy(m).wait_recv()
                        q1_rim(m).start()
                    send_1(0)

                q1_rim(n).wait_recv()

        with jax.named_scope("solve_1"):
            solve(n, cx // 2, c1)

        cross(2, n).start()

        @pl.when(n == 1)
        def _():
            send_1(1)

    def send_1(n):
        @pl.when(has_right)
        def _():
            for copy in c1_copies(n):
                copy.start()

    def look_1(n):
        img_rim(n).wait_send()
        with jax.named_scope("image_1"):
            sums = image(n, c1, 3, cx + 1, (zero,) * 4, True)
            cross(4, n).start()

        @pl.when(has_left)
        def _():
            with jax.named_scope("c1_wait"):
                for copy in c1_copies(n):
                    copy.wait_recv()

        with jax.named_scope("image_1"):
            cross(3, n).start()
            sums = image(n, c1, 1, 3, sums, True)
            share(1, n, row_of(sums[:2]))
            cross(5, n).start()
        with jax.named_scope("squares"):
            share(2, n, squares(n, sums[2], sums[3]))

    def finish_1(m):
        with jax.named_scope("total_1"):
            pick = totals(1, m)
            alpha = pick(0) / pick(1)
            start = al[m]
        with jax.named_scope("cross_wait"):
            for k in range(6):
                cross(k, m).wait_recv()

        def body(j, carry):
            r = pl.multiple_of(own + j * ROWS, ROWS)
            here = pl.ds(r, ROWS)
            there = pl.ds(r + PAD, ROWS)
            step = pl.ds(pl.multiple_of(j * ROWS, ROWS), ROWS)
            near = pl.ds(pl.multiple_of(colour * own_rows + j * ROWS, ROWS), ROWS)
            far = pl.ds(pl.multiple_of((1 - colour) * own_rows + j * ROWS, ROWS), ROWS)
            for p in range(cx):
                for i in range(half):
                    t = colour * half + i
                    u = start * c0[m, p + 1, t, there, :] + alpha * c1[m, p + 1, t, there, :]
                    sol[m, p, near, lane(i)] = u
                    value = q[m, p + 1, t, here, :] - alpha * img[m, p, t, here, :]
                    res[m, p, near, lane(i)] = value
                    u = start * x_c0[m, p, i, step, :] + alpha * x_c1[m, p, i, step, :]
                    sol[m, p, far, lane(i)] = u
                    value = x_q[m, p, i, step, :] - alpha * x_img[m, p, i, step, :]
                    res[m, p, far, lane(i)] = value
            return carry

        with jax.named_scope("finish"):
            lax.fori_loop(0, own_rows // ROWS, body, 0, unroll=2)
        with jax.named_scope("norm"):
            norm_row[...] = jnp.where(at[0:1] == m, norm_of(m, alpha), norm_row[...])

    norm_row[...] = jnp.zeros((1, LANES), jnp.float32)
    pipeline(solve_1, send_1, look_1, finish_1)
    norms[...] = norm_row[0, 0:nrhs]

    with jax.named_scope("drain"):

        @pl.when(has_right)
        def _():
            arrived(dg.at[0, :, q_rows], q_send.at[nrhs])
            for n in range(nrhs):
                q1_rim(n).wait_send()
                c0_rim(n).wait_send()
                for copy in c1_copies(n):
                    copy.wait_send()

        @pl.when(has_left)
        def _():
            arrived(dg.at[cx + 1, :, q_rows], d_send)
            for n in range(nrhs):
                q_rim(n).wait_send()
                q_copy(n).wait_send()
                for copy in c0_copies(n):
                    copy.wait_send()

        for n in range(nrhs):
            for k in range(3):
                arrived(slots.at[k, n, pl.ds(0, everyone - 1)], a_send.at[k, n])
            for k in range(6):
                cross(k, n).wait_send()


def store_kernel(sol_in, res_in, norms_in, sol, res, norms, sems):
    copies = []
    for n in range(sol.shape[0]):
        for src, dst in ((sol_in, sol), (res_in, res)):
            copies.append(pltpu.make_async_copy(src.at[n], dst.at[n], sems.at[len(copies)]))
    copies.append(pltpu.make_async_copy(norms_in, norms, sems.at[len(copies)]))
    for copy in copies:
        copy.start()
    for copy in copies:
        copy.wait()


def shards(rhs, diagonal):
    count = lax.axis_size("sub")
    nrhs, cx, ny, nz = rhs.shape
    assert cx == 4 and SWEEPS % 2 == 0
    tiles = nz // LANES
    rows = ny // 2 + RIM
    padded = rows + 2 * PAD
    f32 = jnp.float32
    out = jax.ShapeDtypeStruct((nrhs, cx, ny, nz // 2), f32)
    dma = pltpu.SemaphoreType.DMA
    crossed = pltpu.VMEM((nrhs, cx, tiles // 2, ny // 2, LANES), f32)
    remote = pl.BlockSpec(memory_space=pltpu.HBM)
    near = pl.BlockSpec(memory_space=pltpu.VMEM)
    sol, res, norms = pl.pallas_call(
        functools.partial(kernel, count),
        out_shape=(out, out, jax.ShapeDtypeStruct((nrhs,), f32)),
        in_specs=[remote, remote],
        out_specs=(near, near, near),
        scratch_shapes=[
            pltpu.VMEM((nrhs, cx + 2, tiles, rows, LANES), f32),
            pltpu.VMEM((nrhs, cx + 2, tiles, padded, LANES), f32),
            pltpu.VMEM((nrhs, cx + 2, tiles, padded, LANES), f32),
            pltpu.VMEM((nrhs, cx, tiles, rows, LANES), f32),
            pltpu.VMEM((cx + 2, tiles, rows, LANES), f32),
            pltpu.VMEM((cx + 2, tiles, rows, LANES), f32),
            pltpu.VMEM((2, cx // 2 + 2, tiles, padded, LANES), f32),
            pltpu.VMEM((nrhs, ROWS, LANES), f32),
            pltpu.VMEM((3, nrhs, 2 * count, 1, LANES), f32),
            pltpu.VMEM((3, nrhs, 1, LANES), f32),
            crossed, crossed, crossed, crossed,
            pltpu.VMEM((1, LANES), f32),
            dma((nrhs + 1,)),
            dma((nrhs + 1,)), dma((nrhs + 1,)),
            dma, dma,
            dma((2, nrhs, 2)), dma((2, nrhs, 2)),
            dma((nrhs,)), dma((nrhs,)),
            dma((nrhs,)), dma((nrhs,)),
            dma((3, nrhs)), dma((3, nrhs)),
            dma((2 + 3 * nrhs,)), dma((2 + 3 * nrhs,)),
            dma((nrhs, 6)), dma((nrhs, 6)),
        ],
        compiler_params=pltpu.CompilerParams(
            collective_id=0, has_side_effects=True, vmem_limit_bytes=44 << 20
        ),
        name="schwarz",
    )(
        pltpu.with_memory_space_constraint(rhs, pltpu.HBM),
        pltpu.with_memory_space_constraint(diagonal, pltpu.HBM),
    )
    return pl.pallas_call(
        store_kernel,
        out_shape=(out, out, jax.ShapeDtypeStruct((nrhs,), f32)),
        in_specs=[pl.BlockSpec(memory_space=pl.ANY)] * 3,
        out_specs=(remote, remote, remote),
        scratch_shapes=[dma((2 * nrhs + 1,))],
        compiler_params=pltpu.CompilerParams(vmem_limit_bytes=1 << 20),
        name="store",
    )(sol, res, norms)


def solution(mesh):
    placed = (P(None, "sub", None, None), P("sub", None, None))
    return jax.shard_map(
        shards,
        mesh=mesh,
        in_specs=placed,
        out_specs=(P(None, "sub", None, "colour"), P(None, "sub", None, "colour"), P()),
        check_vma=False,
    )
```

```python
import functools

import jax
import jax.numpy as jnp
from jax import lax
from jax.experimental import pallas as pl
from jax.experimental.pallas import tpu as pltpu
from jax.sharding import PartitionSpec as P

SWEEPS = 8
OMEGA = 0.8
ROWS = 8
LANES = 128
RIM = 8
PAD = 8
MESH = pl.DeviceIdType.MESH


def lane(t):
    return slice(t * LANES, (t + 1) * LANES)


def beside_lanes(at, row, t):
    zero = jnp.zeros_like(row[t])
    low = row[t - 1] if t > 0 else zero
    high = row[t + 1] if t + 1 < len(row) else zero
    left = pltpu.roll(jnp.where(at == LANES - 1, low, row[t]), 1, 1)
    right = pltpu.roll(jnp.where(at == 0, high, row[t]), LANES - 1, 1)
    return left + right


def kernel(
    count, rhs, diagonal, sol, res, norms, q, c0, c1, img, dg, sc, e, al, slots, mine,
    x_c0, x_q, x_c1, x_img,
    load_sem, q_send, q_recv, d_send, d_recv, c_send, c_recv, u_send, u_recv, r_send, r_recv,
    a_send, a_recv, f_send, f_recv, x_send, x_recv,
):
    colour = lax.axis_index("colour")
    sub = lax.axis_index("sub")
    nrhs, cx, ny, nz = rhs.shape
    span = cx // 2 + 2
    tiles = nz // LANES
    own_rows = ny // 2
    rows = own_rows + RIM
    begin = pl.multiple_of(colour * (own_rows - RIM), ROWS)
    own = pl.multiple_of(colour * RIM, ROWS)
    everyone = 2 * count
    me = colour * count + sub
    has_left = sub > 0
    has_right = sub < count - 1
    left = (colour, sub - 1)
    right = (colour, sub + 1)
    partner = (1 - colour, sub)
    at = lax.broadcasted_iota(jnp.int32, (ROWS, LANES), 1)

    core_rows = pl.ds(pl.multiple_of(colour * own_rows, ROWS), own_rows)
    q_rows = pl.ds(own, own_rows)
    edge_rows = pl.ds(PAD + own, own_rows)

    def hbm(t):
        return (slice(None), pl.ds(begin, rows), lane(t))

    barrier = pltpu.get_barrier_semaphore()

    def every_peer(act):
        for other, first in ((colour, 1), (1 - colour, 0)):

            def body(i, carry):
                act((other, lax.rem(sub + i, count)))
                return carry

            lax.fori_loop(first, count, body, 0, unroll=3 if first else 4)

    every_peer(
        lambda to: pl.semaphore_signal(barrier, inc=1, device_id=to, device_id_type=MESH)
    )

    def arrived(ref, sem):
        pltpu.make_async_copy(ref, ref, sem).wait()

    for t in range(tiles):
        pltpu.make_async_copy(
            diagonal.at[hbm(t)], dg.at[1 : cx + 1, t], load_sem.at[nrhs]
        ).start()
    for n in range(nrhs):
        for t in range(tiles):
            pltpu.make_async_copy(
                rhs.at[(n,) + hbm(t)], q.at[n, 1 : cx + 1, t], load_sem.at[n]
            ).start()

    zero = jnp.zeros((ROWS, LANES), jnp.float32)
    for t in range(tiles):
        for edge in (0, PAD + rows):
            for k in range(2):
                for p in range(span):
                    e[k, p, t, edge : edge + ROWS, :] = zero
            for n in range(nrhs):
                for p in range(cx + 2):
                    c0[n, p, t, edge : edge + ROWS, :] = zero
                    c1[n, p, t, edge : edge + ROWS, :] = zero

    def clear(ref, index, offset):
        def body(j, carry):
            r = pl.multiple_of(offset + j * ROWS, ROWS)
            for t in range(tiles):
                ref[index + (t, pl.ds(r, ROWS), slice(None))] = zero
            return carry

        lax.fori_loop(0, rows // ROWS, body, 0)

    @pl.when(jnp.logical_not(has_left))
    def _():
        clear(sc, (0,), 0)
        for n in range(nrhs):
            clear(q, (n, 0), 0)
            clear(c1, (n, 0), PAD)
            clear(c1, (n, 1), PAD)

    @pl.when(jnp.logical_not(has_right))
    def _():
        clear(sc, (cx + 1,), 0)
        clear(dg, (cx + 1,), 0)
        for n in range(nrhs):
            clear(q, (n, cx + 1), 0)
            clear(c0, (n, cx), PAD)
            clear(c0, (n, cx + 1), PAD)

    arrived(dg.at[1 : cx + 1], load_sem.at[nrhs])
    with jax.named_scope("barrier"):
        pl.semaphore_wait(barrier, everyone - 1)

    def send(src, dst, send_sem, recv_sem, to):
        return pltpu.make_async_remote_copy(
            src_ref=src, dst_ref=dst, send_sem=send_sem, recv_sem=recv_sem,
            device_id=to, device_id_type=MESH,
        )

    @pl.when(has_right)
    def _():
        send(
            dg.at[cx, :, q_rows], dg.at[0, :, q_rows],
            q_send.at[nrhs], q_recv.at[nrhs], right,
        ).start()
        for n in range(nrhs):
            for t in range(tiles):
                send(
                    rhs.at[n, cx - 1, core_rows, lane(t)], q.at[n, 0, t, q_rows],
                    q_send.at[n], q_recv.at[n], right,
                ).start()

    rim_from = (1 - colour) * (own_rows - RIM) + colour * RIM
    rim_to = colour * own_rows

    def rim_copy(ref, pad, send_sem, recv_sem):
        return send(
            ref.at[..., pl.ds(pl.multiple_of(rim_from + pad, ROWS), RIM), :],
            ref.at[..., pl.ds(pl.multiple_of(rim_to + pad, ROWS), RIM), :],
            send_sem, recv_sem, partner,
        )

    def img_rim(n):
        return rim_copy(img.at[n], 0, r_send.at[n], r_recv.at[n])

    def q_rim(n):
        return rim_copy(q.at[n, 0], 0, f_send.at[2 + n], f_recv.at[2 + n])

    def q1_rim(n):
        k = 2 + nrhs + n
        return rim_copy(q.at[n, cx + 1], 0, f_send.at[k], f_recv.at[k])

    def c0_rim(n):
        k = 2 + 2 * nrhs + n
        return rim_copy(c0.at[n, cx], PAD, f_send.at[k], f_recv.at[k])

    def c1_rim(n):
        k = 2 + 3 * nrhs + n
        return rim_copy(c1.at[n, 1], PAD, f_send.at[k], f_recv.at[k])

    half = tiles // 2
    away = pl.ds((1 - colour) * half, half)

    def cross(k, n):
        src, dst = (
            (c0.at[n, 1 : cx + 1, away, edge_rows], x_c0.at[n]),
            (q.at[n, 1 : cx + 1, away, q_rows], x_q.at[n]),
            (c1.at[n, 1 : cx + 1, away, edge_rows], x_c1.at[n]),
            (img.at[n, 1:cx, away, q_rows], x_img.at[n, 1:cx]),
            (img.at[n, 0:1, away, q_rows], x_img.at[n, 0:1]),
        )[k]
        if k == 4:
            return send(src, dst, r_send.at[n], r_recv.at[n], partner)
        k = max(k - 1, 0)
        return send(src, dst, x_send.at[n, k], x_recv.at[n, k], partner)

    def cross_done(k, n, sem):
        ref = (q.at[n, 0:cx, :, q_rows], x_c1.at[n], x_img.at[n, 1:cx])[k]
        arrived(ref, sem.at[n, k])

    def scale_of(low, high):
        def body(j, carry):
            here = pl.ds(pl.multiple_of(j * ROWS, ROWS), ROWS)
            for p in range(low, high):
                for t in range(tiles):
                    sc[p, t, here, :] = OMEGA / (6.0 + dg[p, t, here, :])
            return carry

        lax.fori_loop(0, rows // ROWS, body, 0)

    scale_of(1, cx + 1)

    @pl.when(has_left)
    def _():
        with jax.named_scope("d_wait"):
            arrived(dg.at[0, :, q_rows], q_recv.at[nrhs])
            copy = rim_copy(dg.at[0], 0, f_send.at[0], f_recv.at[0])
            copy.start()
            copy.wait()
            scale_of(0, 1)

    def solve(n, base, out):
        def first(j, carry):
            r = pl.multiple_of(j * ROWS, ROWS)
            here = pl.ds(r, ROWS)
            for p in range(span):
                for t in range(tiles):
                    e[0, p, t, pl.ds(r + PAD, ROWS), :] = (
                        sc[base + p, t, here, :] * q[n, base + p, t, here, :]
                    )
            return carry

        lax.fori_loop(0, rows // ROWS, first, 0)

        def sweep(src, write):
            def body(j, carry):
                r = pl.multiple_of(j * ROWS, ROWS)
                here = pl.ds(r, ROWS)
                planes = [
                    [e[src, p, t, pl.ds(r + PAD, ROWS), :] for t in range(tiles)]
                    for p in range(span)
                ]
                for p in range(span):
                    for t in range(tiles):
                        total = e[src, p, t, pl.ds(r + PAD - 1, ROWS), :]
                        total = total + e[src, p, t, pl.ds(r + PAD + 1, ROWS), :]
                        if p > 0:
                            total = total + planes[p - 1][t]
                        if p + 1 < span:
                            total = total + planes[p + 1][t]
                        total = total + beside_lanes(at, planes[p], t)
                        total = total + q[n, base + p, t, here, :]
                        value = (1.0 - OMEGA) * planes[p][t]
                        write(p, t, r, value + sc[base + p, t, here, :] * total)
                return carry

            lax.fori_loop(0, rows // ROWS, body, 0, unroll=True)

        def into(dst):
            def write(p, t, r, value):
                e[dst, p, t, pl.ds(r + PAD, ROWS), :] = value

            return write

        def write_out(p, t, r, value):
            out[n, base + p, t, pl.ds(r + PAD, ROWS), :] = value

        def two(s, carry):
            sweep(0, into(1))
            sweep(1, into(0))
            return carry

        lax.fori_loop(0, (SWEEPS - 2) // 2, two, 0)
        sweep(0, write_out)

    def image(n, c, low, high, sums):
        def body(j, carry):
            r = pl.multiple_of(own + j * ROWS, ROWS)
            here = pl.ds(r, ROWS)
            sums = list(carry)
            planes = {
                p: [c[n, p, t, pl.ds(r + PAD, ROWS), :] for t in range(tiles)]
                for p in range(low - 1, high + 1)
            }
            for p in range(low, high):
                for t in range(tiles):
                    total = c[n, p, t, pl.ds(r + PAD - 1, ROWS), :]
                    total = total + c[n, p, t, pl.ds(r + PAD + 1, ROWS), :]
                    total = total + planes[p - 1][t] + planes[p + 1][t]
                    total = total + beside_lanes(at, planes[p], t)
                    centre = planes[p][t]
                    value = (6.0 + dg[p, t, here, :]) * centre - total
                    img[n, p - 1, t, here, :] = value
                    mine_q = q[n, p, t, here, :]
                    sums[0] = sums[0] + mine_q * centre
                    sums[1] = sums[1] + centre * value
            return tuple(sums)

        return lax.fori_loop(0, own_rows // ROWS, body, sums, unroll=4)

    def row_of(sums):
        first = lax.broadcasted_iota(jnp.int32, (1, LANES), 1)
        row = jnp.zeros((1, LANES), jnp.float32)
        for i, value in enumerate(sums):
            row = jnp.where(first == i, jnp.sum(value), row)
        return row

    def block(n):
        low, high = cx // 2, cx // 2 + span

        def body(j, carry):
            r = pl.multiple_of(own + j * ROWS, ROWS)
            here = pl.ds(r, ROWS)
            upper, lower = list(carry[0]), list(carry[1])
            planes = {
                p: [c1[n, p, t, pl.ds(r + PAD, ROWS), :] for t in range(tiles)]
                for p in range(low, high)
            }
            for p in range(low, high):
                for t in range(tiles):
                    total = c1[n, p, t, pl.ds(r + PAD - 1, ROWS), :]
                    total = total + c1[n, p, t, pl.ds(r + PAD + 1, ROWS), :]
                    if p > low:
                        total = total + planes[p - 1][t]
                    if p + 1 < high:
                        total = total + planes[p + 1][t]
                    total = total + beside_lanes(at, planes[p], t)
                    centre = planes[p][t]
                    value = (6.0 + dg[p, t, here, :]) * centre - total
                    if p <= cx:
                        img[n, p - 1, t, here, :] = value
                    upper[p - low] = upper[p - low] + q[n, p, t, here, :] * centre
                    lower[p - low] = lower[p - low] + centre * value
            return tuple(upper), tuple(lower)

        return lax.fori_loop(
            0, own_rows // ROWS, body, ((zero,) * span, (zero,) * span), unroll=4
        )

    def couple(n):
        first = cx // 2

        def body(j, total):
            r = pl.multiple_of(own + j * ROWS, ROWS)
            here = pl.ds(r, ROWS)
            for t in range(tiles):
                beside = c1[n, first - 1, t, pl.ds(r + PAD, ROWS), :]
                total = total + beside * c1[n, first, t, pl.ds(r + PAD, ROWS), :]
                img[n, first - 1, t, here, :] = img[n, first - 1, t, here, :] - beside
            return total

        return lax.fori_loop(0, own_rows // ROWS, body, zero, unroll=4)

    def edge(n, alpha, total):
        def body(j, total):
            r = pl.multiple_of(own + j * ROWS, ROWS)
            here = pl.ds(r, ROWS)
            there = pl.ds(r + PAD, ROWS)
            row = [c1[n, 1, t, there, :] for t in range(tiles)]
            for t in range(tiles):
                around = c1[n, 1, t, pl.ds(r + PAD - 1, ROWS), :]
                around = around + c1[n, 1, t, pl.ds(r + PAD + 1, ROWS), :]
                around = around + c1[n, 0, t, there, :] + c1[n, 2, t, there, :]
                around = around + beside_lanes(at, row, t)
                value = (6.0 + dg[1, t, here, :]) * row[t] - around
                img[n, 0, t, here, :] = value
                rest = q[n, 1, t, here, :] - alpha * value
                total = total + rest * rest
            return total

        return lax.fori_loop(0, own_rows // ROWS, body, total, unroll=4)

    def squares(n, alpha):
        def body(j, carry):
            here = pl.ds(pl.multiple_of(own + j * ROWS, ROWS), ROWS)
            sums = list(carry)
            for p in range(1, cx):
                for t in range(tiles):
                    rest = q[n, p + 1, t, here, :] - alpha * img[n, p, t, here, :]
                    sums[p - 1] = sums[p - 1] + rest * rest
            return tuple(sums)

        return sum(lax.fori_loop(0, own_rows // ROWS, body, (zero,) * (cx - 1), unroll=2))

    def share(k, n, row):
        mine[k, n] = row
        slots[k, n, me] = row

        every_peer(
            lambda to: send(
                mine.at[k, n], slots.at[k, n, me], a_send, a_recv.at[k, n], to
            ).start()
        )

    def totals(k, n):
        arrived(slots.at[k, n, pl.ds(0, everyone - 1)], a_recv.at[k, n])
        row = jnp.sum(slots[k, n], axis=0)
        first = lax.broadcasted_iota(jnp.int32, (1, LANES), 1)

        def pick(i):
            value = jnp.sum(jnp.where(first == i, row, 0.0), axis=1, keepdims=True)
            return jnp.broadcast_to(value, (ROWS, LANES))

        return pick

    def c0_copy(n):
        return send(
            c0.at[n, 0:2, :, edge_rows], c0.at[n, cx : cx + 2, :, edge_rows],
            c_send.at[n, 2], c_recv.at[n, 2], left,
        )

    def c1_copy(n, k):
        return send(
            c1.at[n, cx + 1 - k, :, edge_rows], c1.at[n, 1 - k, :, edge_rows],
            c_send.at[n, k], c_recv.at[n, k], right,
        )

    def q_copy(n):
        return send(
            q.at[n, 1, :, q_rows], q.at[n, cx + 1, :, q_rows], u_send.at[n], u_recv.at[n], left
        )

    def pipeline(solve_one, send_one, look_one, finish_one):
        def body(k, carry):
            @pl.when(k < nrhs)
            def _():
                solve_one(k)

            @pl.when((k >= 2) & (k < nrhs + 2))
            def _():
                look_one(k - 2)

            @pl.when((k >= 2) & (k < nrhs))
            def _():
                send_one(k)

            @pl.when(k >= 3)
            def _():
                finish_one(k - 3)

            return carry

        lax.fori_loop(0, nrhs + 3, body, 0)

    def q_here():
        for m in range(1, nrhs):
            arrived(q.at[m, 0, :, q_rows], q_recv.at[m])

    def solve_0(n):
        arrived(q.at[n, 1 : cx + 1], load_sem.at[n])

        @pl.when(n == 1)
        def _():
            with jax.named_scope("gate_0"):

                @pl.when(has_right)
                def _():
                    for m in range(nrhs):
                        arrived(q.at[m, 0, :, q_rows], q_send.at[m])

                @pl.when(jnp.logical_not(has_right))
                def _():
                    q_here()

                @pl.when(has_left)
                def _():
                    send(
                        dg.at[1, :, q_rows], dg.at[cx + 1, :, q_rows], d_send, d_recv, left
                    ).start()

                send_0(0)

                @pl.when(has_right & has_left)
                def _():
                    q_here()

                @pl.when(has_left)
                def _():
                    for m in range(1, nrhs):
                        q_rim(m).start()

        @pl.when(has_left)
        def _():
            with jax.named_scope("q_wait"):

                @pl.when(n == 0)
                def _():
                    arrived(q.at[0, 0, :, q_rows], q_recv.at[0])
                    q_rim(0).start()

                q_rim(n).wait_recv()

        with jax.named_scope("solve_0"):
            solve(n, 0, c0)

        @pl.when(n == 1)
        def _():
            send_0(1)

    def send_0(n):
        @pl.when(has_left)
        def _():
            c0_copy(n).start()

    def look_0(n):
        with jax.named_scope("image_0"):
            sums = image(n, c0, 1, cx - 1, (zero,) * 2)

        @pl.when(has_right)
        def _():
            with jax.named_scope("c0_wait"):
                c0_copy(n).wait_recv()
                c0_rim(n).start()
                c0_rim(n).wait_recv()

        with jax.named_scope("image_0"):
            sums = image(n, c0, cx - 1, cx + 1, sums)
            share(0, n, row_of(sums))
            img_rim(n).start()
            cross(0, n).start()

    def finish_0(m):
        with jax.named_scope("total_0"):
            pick = totals(0, m)
            alpha = pick(0) / pick(1)
            al[m] = alpha
        with jax.named_scope("rim_wait"):
            img_rim(m).wait_recv()

        def body(j, carry):
            here = pl.ds(pl.multiple_of(j * ROWS, ROWS), ROWS)
            for p in range(cx):
                for t in range(tiles):
                    value = q[m, p + 1, t, here, :] - alpha * img[m, p, t, here, :]
                    q[m, p + 1, t, here, :] = value
            return carry

        with jax.named_scope("update_0"):
            lax.fori_loop(0, rows // ROWS, body, 0)

        @pl.when(has_left)
        def _():
            q_copy(m).start()

        cross(1, m).start()

    pipeline(solve_0, send_0, look_0, finish_0)

    @pl.when(has_right)
    def _():
        arrived(dg.at[cx + 1, :, q_rows], d_recv)
        copy = rim_copy(dg.at[cx + 1], 0, f_send.at[1], f_recv.at[1])
        copy.start()
        copy.wait()
        scale_of(cx + 1, cx + 2)

    def q1_here():
        for m in range(1, nrhs):
            q_copy(m).wait_recv()

    def solve_1(n, carry):
        @pl.when(has_right)
        def _():
            with jax.named_scope("q1_wait"):

                @pl.when(n == 0)
                def _():
                    q_copy(0).wait_recv()
                    q1_rim(0).start()

                @pl.when(n == 1)
                def _():
                    @pl.when(has_left)
                    def _():
                        for m in range(nrhs):
                            q_copy(m).wait_send()

                    @pl.when(jnp.logical_not(has_left))
                    def _():
                        q1_here()

                    c1_copy(0, 0).start()

                    @pl.when(has_left)
                    def _():
                        q1_here()

                    for m in range(1, nrhs):
                        q1_rim(m).start()

                q1_rim(n).wait_recv()

        with jax.named_scope("solve_1"):
            solve(n, cx // 2, c1)

        @pl.when((n > 0) & has_right)
        def _():
            c1_copy(n, 0).start()

            @pl.when(n == nrhs - 1)
            def _():
                c1_copy(0, 1).start()

        return carry

    lax.fori_loop(0, nrhs, solve_1, 0)

    def look_1(n, carry):
        img_rim(n).wait_send()
        with jax.named_scope("block"):
            upper, lower = block(n)

        @pl.when(has_left)
        def _():
            with jax.named_scope("c1_wait"):
                c1_copy(n, 0).wait_recv()

        with jax.named_scope("couple"):
            both = couple(n)
            share(1, n, row_of((sum(upper), sum(lower) - 2.0 * both)))

        @pl.when((n == nrhs - 1) & has_right)
        def _():
            for m in range(1, nrhs):
                c1_copy(m, 1).start()

        @pl.when(has_left)
        def _():
            c1_rim(n).start()

        cross(2, n).start()
        cross(3, n).start()
        return carry

    lax.fori_loop(0, nrhs, look_1, 0)

    def finish_1(m, carry):
        with jax.named_scope("total_1"):
            pick = totals(1, m)
            alpha = pick(0) / pick(1)
            start = al[m]
        with jax.named_scope("cross_wait"):
            for k in range(3):
                cross_done(k, m, x_recv)

        def update(solution_planes, residual_planes):
            def body(j, carry):
                r = pl.multiple_of(own + j * ROWS, ROWS)
                here = pl.ds(r, ROWS)
                there = pl.ds(r + PAD, ROWS)
                step = pl.ds(pl.multiple_of(j * ROWS, ROWS), ROWS)
                near = pl.ds(pl.multiple_of(colour * own_rows + j * ROWS, ROWS), ROWS)
                far = pl.ds(pl.multiple_of((1 - colour) * own_rows + j * ROWS, ROWS), ROWS)
                for i in range(half):
                    t = colour * half + i
                    for p in solution_planes:
                        u = start * c0[m, p + 1, t, there, :]
                        sol[m, p, near, lane(i)] = u + alpha * c1[m, p + 1, t, there, :]
                        u = start * x_c0[m, p, i, step, :]
                        sol[m, p, far, lane(i)] = u + alpha * x_c1[m, p, i, step, :]
                    for p in residual_planes:
                        value = alpha * img[m, p, t, here, :]
                        res[m, p, near, lane(i)] = q[m, p + 1, t, here, :] - value
                        value = alpha * x_img[m, p, i, step, :]
                        res[m, p, far, lane(i)] = x_q[m, p, i, step, :] - value
                return carry

            lax.fori_loop(0, own_rows // ROWS, body, 0, unroll=2)

        with jax.named_scope("finish"):
            update(range(cx), range(1, cx))
            total = squares(m, alpha)

        @pl.when(has_left)
        def _():
            with jax.named_scope("edge_wait"):
                c1_rim(m).wait_recv()
                c1_copy(m, 1).wait_recv()

        with jax.named_scope("edge"):
            total = edge(m, alpha, total)
            cross(4, m).start()
            share(2, m, row_of((total,)))
            cross(4, m).wait_recv()
            update((), (0,))
        return carry

    lax.fori_loop(0, nrhs, finish_1, 0)

    with jax.named_scope("norm"):
        found = jnp.zeros((1, LANES), jnp.float32)
        for n in range(nrhs):
            square = totals(2, n)(0)[0:1]
            found = jnp.where(at[0:1] == n, jnp.sqrt(square), found)
        norms[...] = found[0, 0:nrhs]

    with jax.named_scope("drain"):

        @pl.when(has_right)
        def _():
            arrived(dg.at[0, :, q_rows], q_send.at[nrhs])
            for n in range(nrhs):
                q1_rim(n).wait_send()
                c0_rim(n).wait_send()
                for k in range(2):
                    c1_copy(n, k).wait_send()

        @pl.when(has_left)
        def _():
            arrived(dg.at[cx + 1, :, q_rows], d_send)
            for n in range(nrhs):
                q_rim(n).wait_send()
                c1_rim(n).wait_send()
                c0_copy(n).wait_send()

        @pl.when(has_left & jnp.logical_not(has_right))
        def _():
            for n in range(nrhs):
                q_copy(n).wait_send()

        arrived(slots.at[:, :, pl.ds(0, everyone - 1)], a_send)
        for n in range(nrhs):
            for k in range(3):
                cross_done(k, n, x_send)
            cross(4, n).wait_send()


def store_kernel(sol_in, res_in, norms_in, sol, res, norms, sems):
    copies = []
    for n in range(sol.shape[0]):
        for src, dst in ((sol_in, sol), (res_in, res)):
            copies.append(pltpu.make_async_copy(src.at[n], dst.at[n], sems.at[len(copies)]))
    copies.append(pltpu.make_async_copy(norms_in, norms, sems.at[len(copies)]))
    for copy in copies:
        copy.start()
    for copy in copies:
        copy.wait()


def shards(rhs, diagonal):
    count = lax.axis_size("sub")
    nrhs, cx, ny, nz = rhs.shape
    assert cx == 4 and SWEEPS % 2 == 0
    tiles = nz // LANES
    rows = ny // 2 + RIM
    padded = rows + 2 * PAD
    f32 = jnp.float32
    out = jax.ShapeDtypeStruct((nrhs, cx, ny, nz // 2), f32)
    dma = pltpu.SemaphoreType.DMA
    crossed = pltpu.VMEM((nrhs, cx, tiles // 2, ny // 2, LANES), f32)
    remote = pl.BlockSpec(memory_space=pltpu.HBM)
    near = pl.BlockSpec(memory_space=pltpu.VMEM)
    sol, res, norms = pl.pallas_call(
        functools.partial(kernel, count),
        out_shape=(out, out, jax.ShapeDtypeStruct((nrhs,), f32)),
        in_specs=[remote, remote],
        out_specs=(near, near, near),
        scratch_shapes=[
            pltpu.VMEM((nrhs, cx + 2, tiles, rows, LANES), f32),
            pltpu.VMEM((nrhs, cx + 2, tiles, padded, LANES), f32),
            pltpu.VMEM((nrhs, cx + 2, tiles, padded, LANES), f32),
            pltpu.VMEM((nrhs, cx, tiles, rows, LANES), f32),
            pltpu.VMEM((cx + 2, tiles, rows, LANES), f32),
            pltpu.VMEM((cx + 2, tiles, rows, LANES), f32),
            pltpu.VMEM((2, cx // 2 + 2, tiles, padded, LANES), f32),
            pltpu.VMEM((nrhs, ROWS, LANES), f32),
            pltpu.VMEM((3, nrhs, 2 * count, 1, LANES), f32),
            pltpu.VMEM((3, nrhs, 1, LANES), f32),
            crossed, crossed, crossed, crossed,
            dma((nrhs + 1,)),
            dma((nrhs + 1,)), dma((nrhs + 1,)),
            dma, dma,
            dma((nrhs, 3)), dma((nrhs, 3)),
            dma((nrhs,)), dma((nrhs,)),
            dma((nrhs,)), dma((nrhs,)),
            dma, dma((3, nrhs)),
            dma((2 + 4 * nrhs,)), dma((2 + 4 * nrhs,)),
            dma((nrhs, 3)), dma((nrhs, 3)),
        ],
        compiler_params=pltpu.CompilerParams(
            collective_id=0, has_side_effects=True, vmem_limit_bytes=44 << 20
        ),
        name="schwarz",
    )(
        pltpu.with_memory_space_constraint(rhs, pltpu.HBM),
        pltpu.with_memory_space_constraint(diagonal, pltpu.HBM),
    )
    return pl.pallas_call(
        store_kernel,
        out_shape=(out, out, jax.ShapeDtypeStruct((nrhs,), f32)),
        in_specs=[pl.BlockSpec(memory_space=pl.ANY)] * 3,
        out_specs=(remote, remote, remote),
        scratch_shapes=[dma((2 * nrhs + 1,))],
        compiler_params=pltpu.CompilerParams(vmem_limit_bytes=1 << 20),
        name="store",
    )(sol, res, norms)


def solution(mesh):
    placed = (P(None, "sub", None, None), P("sub", None, None))
    return jax.shard_map(
        shards,
        mesh=mesh,
        in_specs=placed,
        out_specs=(P(None, "sub", None, "colour"), P(None, "sub", None, "colour"), P()),
        check_vma=False,
    )
```

```python
import functools

import jax
import jax.numpy as jnp
from jax import lax
from jax.experimental import pallas as pl
from jax.experimental.pallas import tpu as pltpu
from jax.sharding import PartitionSpec as P

SWEEPS = 8
OMEGA = 0.8
ROWS = 8
LANES = 128
RIM = 8
PAD = 8
MESH = pl.DeviceIdType.MESH


def lane(t):
    return slice(t * LANES, (t + 1) * LANES)


def beside_lanes(at, row, t):
    zero = jnp.zeros_like(row[t])
    low = row[t - 1] if t > 0 else zero
    high = row[t + 1] if t + 1 < len(row) else zero
    left = pltpu.roll(jnp.where(at == LANES - 1, low, row[t]), 1, 1)
    right = pltpu.roll(jnp.where(at == 0, high, row[t]), LANES - 1, 1)
    return left + right


def kernel(
    count, rhs, diagonal, sol, res, norms, q, c0, c1, img, dg, sc, e, al, slots, mine,
    x_c0, x_q, x_c1, x_img,
    load_sem, q_send, q_recv, d_send, d_recv, c_send, c_recv, u_send, u_recv, r_send, r_recv,
    a_send, a_recv, f_send, f_recv, x_send, x_recv,
):
    colour = lax.axis_index("colour")
    sub = lax.axis_index("sub")
    nrhs, cx, ny, nz = rhs.shape
    span = cx // 2 + 2
    tiles = nz // LANES
    own_rows = ny // 2
    rows = own_rows + RIM
    begin = pl.multiple_of(colour * (own_rows - RIM), ROWS)
    own = pl.multiple_of(colour * RIM, ROWS)
    everyone = 2 * count
    me = colour * count + sub
    has_left = sub > 0
    has_right = sub < count - 1
    left = (colour, sub - 1)
    right = (colour, sub + 1)
    partner = (1 - colour, sub)
    at = lax.broadcasted_iota(jnp.int32, (ROWS, LANES), 1)

    core_rows = pl.ds(pl.multiple_of(colour * own_rows, ROWS), own_rows)
    q_rows = pl.ds(own, own_rows)
    edge_rows = pl.ds(PAD + own, own_rows)

    def hbm(t):
        return (slice(None), pl.ds(begin, rows), lane(t))

    barrier = pltpu.get_barrier_semaphore()

    def every_peer(act):
        for other, first in ((colour, 1), (1 - colour, 0)):

            def body(i, carry):
                act((other, lax.rem(sub + i, count)))
                return carry

            lax.fori_loop(first, count, body, 0, unroll=3 if first else 4)

    every_peer(
        lambda to: pl.semaphore_signal(barrier, inc=1, device_id=to, device_id_type=MESH)
    )

    def arrived(ref, sem):
        pltpu.make_async_copy(ref, ref, sem).wait()

    for t in range(tiles):
        pltpu.make_async_copy(
            diagonal.at[hbm(t)], dg.at[1 : cx + 1, t], load_sem.at[nrhs]
        ).start()
    for n in range(nrhs):
        for t in range(tiles):
            pltpu.make_async_copy(
                rhs.at[(n,) + hbm(t)], q.at[n, 1 : cx + 1, t], load_sem.at[n]
            ).start()

    zero = jnp.zeros((ROWS, LANES), jnp.float32)
    for t in range(tiles):
        for edge in (0, PAD + rows):
            for k in range(2):
                for p in range(span):
                    e[k, p, t, edge : edge + ROWS, :] = zero
            for n in range(nrhs):
                for p in range(cx + 2):
                    c0[n, p, t, edge : edge + ROWS, :] = zero
                    c1[n, p, t, edge : edge + ROWS, :] = zero

    def clear(ref, index, offset):
        def body(j, carry):
            r = pl.multiple_of(offset + j * ROWS, ROWS)
            for t in range(tiles):
                ref[index + (t, pl.ds(r, ROWS), slice(None))] = zero
            return carry

        lax.fori_loop(0, rows // ROWS, body, 0)

    @pl.when(jnp.logical_not(has_left))
    def _():
        clear(sc, (0,), 0)
        for n in range(nrhs):
            clear(q, (n, 0), 0)
            clear(c1, (n, 0), PAD)
            clear(c1, (n, 1), PAD)

    @pl.when(jnp.logical_not(has_right))
    def _():
        clear(sc, (cx + 1,), 0)
        clear(dg, (cx + 1,), 0)
        for n in range(nrhs):
            clear(q, (n, cx + 1), 0)
            clear(c0, (n, cx), PAD)
            clear(c0, (n, cx + 1), PAD)

    arrived(dg.at[1 : cx + 1], load_sem.at[nrhs])
    with jax.named_scope("barrier"):
        pl.semaphore_wait(barrier, everyone - 1)

    def send(src, dst, send_sem, recv_sem, to):
        return pltpu.make_async_remote_copy(
            src_ref=src, dst_ref=dst, send_sem=send_sem, recv_sem=recv_sem,
            device_id=to, device_id_type=MESH,
        )

    @pl.when(has_right)
    def _():
        send(
            dg.at[cx, :, q_rows], dg.at[0, :, q_rows],
            q_send.at[nrhs], q_recv.at[nrhs], right,
        ).start()
        for n in range(nrhs):
            for t in range(tiles):
                send(
                    rhs.at[n, cx - 1, core_rows, lane(t)], q.at[n, 0, t, q_rows],
                    q_send.at[n], q_recv.at[n], right,
                ).start()

    rim_from = (1 - colour) * (own_rows - RIM) + colour * RIM
    rim_to = colour * own_rows

    def rim_copy(ref, pad, send_sem, recv_sem):
        return send(
            ref.at[..., pl.ds(pl.multiple_of(rim_from + pad, ROWS), RIM), :],
            ref.at[..., pl.ds(pl.multiple_of(rim_to + pad, ROWS), RIM), :],
            send_sem, recv_sem, partner,
        )

    def img_rim(n):
        return rim_copy(img.at[n], 0, r_send.at[n], r_recv.at[n])

    def q_rim(n):
        return rim_copy(q.at[n, 0], 0, f_send.at[2 + n], f_recv.at[2 + n])

    def q1_rim(n):
        k = 2 + nrhs + n
        return rim_copy(q.at[n, cx + 1], 0, f_send.at[k], f_recv.at[k])

    def c0_rim(n):
        k = 2 + 2 * nrhs + n
        return rim_copy(c0.at[n, cx], PAD, f_send.at[k], f_recv.at[k])

    def c1_rim(n):
        k = 2 + 3 * nrhs + n
        return rim_copy(c1.at[n, 1], PAD, f_send.at[k], f_recv.at[k])

    half = tiles // 2
    away = pl.ds((1 - colour) * half, half)

    def cross(k, n):
        src, dst = (
            (c0.at[n, 1 : cx + 1, away, edge_rows], x_c0.at[n]),
            (q.at[n, 1 : cx + 1, away, q_rows], x_q.at[n]),
            (c1.at[n, 1 : cx + 1, away, edge_rows], x_c1.at[n]),
            (img.at[n, 1:cx, away, q_rows], x_img.at[n, 1:cx]),
            (img.at[n, 0:1, away, q_rows], x_img.at[n, 0:1]),
        )[k]
        if k == 4:
            return send(src, dst, r_send.at[n], r_recv.at[n], partner)
        k = max(k - 1, 0)
        return send(src, dst, x_send.at[n, k], x_recv.at[n, k], partner)

    def cross_done(k, n, sem):
        ref = (q.at[n, 0:cx, :, q_rows], x_c1.at[n], x_img.at[n, 1:cx])[k]
        arrived(ref, sem.at[n, k])

    def scale_of(low, high):
        def body(j, carry):
            here = pl.ds(pl.multiple_of(j * ROWS, ROWS), ROWS)
            for p in range(low, high):
                for t in range(tiles):
                    sc[p, t, here, :] = OMEGA / (6.0 + dg[p, t, here, :])
            return carry

        lax.fori_loop(0, rows // ROWS, body, 0)

    scale_of(1, cx + 1)

    @pl.when(has_left)
    def _():
        with jax.named_scope("d_wait"):
            arrived(dg.at[0, :, q_rows], q_recv.at[nrhs])
            copy = rim_copy(dg.at[0], 0, f_send.at[0], f_recv.at[0])
            copy.start()
            copy.wait()
            scale_of(0, 1)

    def solve(n, base, out):
        def first(j, carry):
            r = pl.multiple_of(j * ROWS, ROWS)
            here = pl.ds(r, ROWS)
            for p in range(span):
                for t in range(tiles):
                    e[0, p, t, pl.ds(r + PAD, ROWS), :] = (
                        sc[base + p, t, here, :] * q[n, base + p, t, here, :]
                    )
            return carry

        lax.fori_loop(0, rows // ROWS, first, 0)

        def sweep(src, write):
            def body(j, carry):
                r = pl.multiple_of(j * ROWS, ROWS)
                here = pl.ds(r, ROWS)
                planes = [
                    [e[src, p, t, pl.ds(r + PAD, ROWS), :] for t in range(tiles)]
                    for p in range(span)
                ]
                for p in range(span):
                    for t in range(tiles):
                        total = e[src, p, t, pl.ds(r + PAD - 1, ROWS), :]
                        total = total + e[src, p, t, pl.ds(r + PAD + 1, ROWS), :]
                        if p > 0:
                            total = total + planes[p - 1][t]
                        if p + 1 < span:
                            total = total + planes[p + 1][t]
                        total = total + beside_lanes(at, planes[p], t)
                        total = total + q[n, base + p, t, here, :]
                        value = (1.0 - OMEGA) * planes[p][t]
                        write(p, t, r, value + sc[base + p, t, here, :] * total)
                return carry

            lax.fori_loop(0, rows // ROWS, body, 0, unroll=True)

        def into(dst):
            def write(p, t, r, value):
                e[dst, p, t, pl.ds(r + PAD, ROWS), :] = value

            return write

        def write_out(p, t, r, value):
            out[n, base + p, t, pl.ds(r + PAD, ROWS), :] = value

        def two(s, carry):
            sweep(0, into(1))
            sweep(1, into(0))
            return carry

        lax.fori_loop(0, (SWEEPS - 2) // 2, two, 0)
        sweep(0, write_out)

    def image(n, c, low, high, sums):
        def body(j, carry):
            r = pl.multiple_of(own + j * ROWS, ROWS)
            here = pl.ds(r, ROWS)
            sums = list(carry)
            planes = {
                p: [c[n, p, t, pl.ds(r + PAD, ROWS), :] for t in range(tiles)]
                for p in range(low - 1, high + 1)
            }
            for p in range(low, high):
                for t in range(tiles):
                    total = c[n, p, t, pl.ds(r + PAD - 1, ROWS), :]
                    total = total + c[n, p, t, pl.ds(r + PAD + 1, ROWS), :]
                    total = total + planes[p - 1][t] + planes[p + 1][t]
                    total = total + beside_lanes(at, planes[p], t)
                    centre = planes[p][t]
                    value = (6.0 + dg[p, t, here, :]) * centre - total
                    img[n, p - 1, t, here, :] = value
                    mine_q = q[n, p, t, here, :]
                    sums[0] = sums[0] + mine_q * centre
                    sums[1] = sums[1] + centre * value
            return tuple(sums)

        return lax.fori_loop(0, own_rows // ROWS, body, sums, unroll=4)

    def row_of(sums, start=0, row=None):
        if row is None:
            row = jnp.zeros((1, LANES), jnp.float32)
        for i, value in enumerate(sums):
            row = jnp.where(first_row == start + i, jnp.sum(value), row)
        return row

    def block(n):
        low, high = cx // 2, cx // 2 + span

        def body(j, carry):
            r = pl.multiple_of(own + j * ROWS, ROWS)
            here = pl.ds(r, ROWS)
            upper, lower = list(carry[0]), list(carry[1])
            planes = {
                p: [c1[n, p, t, pl.ds(r + PAD, ROWS), :] for t in range(tiles)]
                for p in range(low, high)
            }
            for p in range(low, high):
                for t in range(tiles):
                    total = c1[n, p, t, pl.ds(r + PAD - 1, ROWS), :]
                    total = total + c1[n, p, t, pl.ds(r + PAD + 1, ROWS), :]
                    if p > low:
                        total = total + planes[p - 1][t]
                    if p + 1 < high:
                        total = total + planes[p + 1][t]
                    total = total + beside_lanes(at, planes[p], t)
                    centre = planes[p][t]
                    value = (6.0 + dg[p, t, here, :]) * centre - total
                    if p <= cx:
                        img[n, p - 1, t, here, :] = value
                    upper[p - low] = upper[p - low] + q[n, p, t, here, :] * centre
                    lower[p - low] = lower[p - low] + centre * value
            return tuple(upper), tuple(lower)

        return lax.fori_loop(
            0, own_rows // ROWS, body, ((zero,) * span, (zero,) * span), unroll=4
        )

    def couple(n):
        first = cx // 2

        def body(j, total):
            r = pl.multiple_of(own + j * ROWS, ROWS)
            here = pl.ds(r, ROWS)
            for t in range(tiles):
                beside = c1[n, first - 1, t, pl.ds(r + PAD, ROWS), :]
                total = total + beside * c1[n, first, t, pl.ds(r + PAD, ROWS), :]
                img[n, first - 1, t, here, :] = img[n, first - 1, t, here, :] - beside
            return total

        return lax.fori_loop(0, own_rows // ROWS, body, zero, unroll=4)

    def edge(n, alpha, total):
        def body(j, total):
            r = pl.multiple_of(own + j * ROWS, ROWS)
            here = pl.ds(r, ROWS)
            there = pl.ds(r + PAD, ROWS)
            row = [c1[n, 1, t, there, :] for t in range(tiles)]
            for t in range(tiles):
                around = c1[n, 1, t, pl.ds(r + PAD - 1, ROWS), :]
                around = around + c1[n, 1, t, pl.ds(r + PAD + 1, ROWS), :]
                around = around + c1[n, 0, t, there, :] + c1[n, 2, t, there, :]
                around = around + beside_lanes(at, row, t)
                value = (6.0 + dg[1, t, here, :]) * row[t] - around
                img[n, 0, t, here, :] = value
                rest = q[n, 1, t, here, :] - alpha * value
                total = total + rest * rest
            return total

        return lax.fori_loop(0, own_rows // ROWS, body, total, unroll=4)

    def squares(n, alpha):
        def body(j, carry):
            here = pl.ds(pl.multiple_of(own + j * ROWS, ROWS), ROWS)
            sums = list(carry)
            for p in range(1, cx):
                for t in range(tiles):
                    rest = q[n, p + 1, t, here, :] - alpha * img[n, p, t, here, :]
                    sums[p - 1] = sums[p - 1] + rest * rest
            return tuple(sums)

        return sum(lax.fori_loop(0, own_rows // ROWS, body, (zero,) * (cx - 1), unroll=2))

    second, third = nrhs, nrhs + 1
    first_row = lax.broadcasted_iota(jnp.int32, (1, LANES), 1)

    def share(k, row):
        mine[k] = row
        slots[k, me] = row

        every_peer(
            lambda to: send(mine.at[k], slots.at[k, me], a_send, a_recv.at[k], to).start()
        )

    def totals(k):
        arrived(slots.at[k, pl.ds(0, everyone - 1)], a_recv.at[k])
        row = jnp.sum(slots[k], axis=0)

        def pick(i):
            value = jnp.sum(jnp.where(first_row == i, row, 0.0), axis=1, keepdims=True)
            return jnp.broadcast_to(value, (ROWS, LANES))

        return pick

    def c0_copy(n):
        return send(
            c0.at[n, 0:2, :, edge_rows], c0.at[n, cx : cx + 2, :, edge_rows],
            c_send.at[n, 2], c_recv.at[n, 2], left,
        )

    def c1_copy(n, k):
        return send(
            c1.at[n, cx + 1 - k, :, edge_rows], c1.at[n, 1 - k, :, edge_rows],
            c_send.at[n, k], c_recv.at[n, k], right,
        )

    def q_copy(n):
        return send(
            q.at[n, 1, :, q_rows], q.at[n, cx + 1, :, q_rows], u_send.at[n], u_recv.at[n], left
        )

    def pipeline(solve_one, send_one, look_one, finish_one):
        def body(k, carry):
            @pl.when(k < nrhs)
            def _():
                solve_one(k)

            @pl.when((k >= 2) & (k < nrhs + 2))
            def _():
                look_one(k - 2)

            @pl.when((k >= 2) & (k < nrhs))
            def _():
                send_one(k)

            @pl.when(k >= 3)
            def _():
                finish_one(k - 3)

            return carry

        lax.fori_loop(0, nrhs + 3, body, 0)

    def q_here():
        for m in range(1, nrhs):
            arrived(q.at[m, 0, :, q_rows], q_recv.at[m])

    def solve_0(n):
        arrived(q.at[n, 1 : cx + 1], load_sem.at[n])

        @pl.when(n == 1)
        def _():
            with jax.named_scope("gate_0"):

                @pl.when(has_right)
                def _():
                    for m in range(nrhs):
                        arrived(q.at[m, 0, :, q_rows], q_send.at[m])

                @pl.when(jnp.logical_not(has_right))
                def _():
                    q_here()

                @pl.when(has_left)
                def _():
                    send(
                        dg.at[1, :, q_rows], dg.at[cx + 1, :, q_rows], d_send, d_recv, left
                    ).start()

                send_0(0)

                @pl.when(has_right & has_left)
                def _():
                    q_here()

                @pl.when(has_left)
                def _():
                    for m in range(1, nrhs):
                        q_rim(m).start()

        @pl.when(has_left)
        def _():
            with jax.named_scope("q_wait"):

                @pl.when(n == 0)
                def _():
                    arrived(q.at[0, 0, :, q_rows], q_recv.at[0])
                    q_rim(0).start()

                q_rim(n).wait_recv()

        with jax.named_scope("solve_0"):
            solve(n, 0, c0)

        @pl.when(n == 1)
        def _():
            send_0(1)

    def send_0(n):
        @pl.when(has_left)
        def _():
            c0_copy(n).start()

    def look_0(n):
        with jax.named_scope("image_0"):
            sums = image(n, c0, 1, cx - 1, (zero,) * 2)

        @pl.when(has_right)
        def _():
            with jax.named_scope("c0_wait"):
                c0_copy(n).wait_recv()
                c0_rim(n).start()
                c0_rim(n).wait_recv()

        with jax.named_scope("image_0"):
            sums = image(n, c0, cx - 1, cx + 1, sums)
            share(n, row_of(sums))
            img_rim(n).start()
            cross(0, n).start()

    def finish_0(m):
        with jax.named_scope("total_0"):
            pick = totals(m)
            alpha = pick(0) / pick(1)
            al[m] = alpha
        with jax.named_scope("rim_wait"):
            img_rim(m).wait_recv()

        def body(j, carry):
            here = pl.ds(pl.multiple_of(j * ROWS, ROWS), ROWS)
            for p in range(cx):
                for t in range(tiles):
                    value = q[m, p + 1, t, here, :] - alpha * img[m, p, t, here, :]
                    q[m, p + 1, t, here, :] = value
            return carry

        with jax.named_scope("update_0"):
            lax.fori_loop(0, rows // ROWS, body, 0)

        @pl.when(has_left)
        def _():
            q_copy(m).start()

        cross(1, m).start()

    pipeline(solve_0, send_0, look_0, finish_0)

    @pl.when(has_right)
    def _():
        arrived(dg.at[cx + 1, :, q_rows], d_recv)
        copy = rim_copy(dg.at[cx + 1], 0, f_send.at[1], f_recv.at[1])
        copy.start()
        copy.wait()
        scale_of(cx + 1, cx + 2)

    def q1_here():
        for m in range(1, nrhs):
            q_copy(m).wait_recv()

    def solve_1(n, carry):
        @pl.when(has_right)
        def _():
            with jax.named_scope("q1_wait"):

                @pl.when(n == 0)
                def _():
                    q_copy(0).wait_recv()
                    q1_rim(0).start()

                @pl.when(n == 1)
                def _():
                    @pl.when(has_left)
                    def _():
                        for m in range(nrhs):
                            q_copy(m).wait_send()

                    @pl.when(jnp.logical_not(has_left))
                    def _():
                        q1_here()

                    c1_copy(0, 0).start()

                    @pl.when(has_left)
                    def _():
                        q1_here()

                    for m in range(1, nrhs):
                        q1_rim(m).start()

                q1_rim(n).wait_recv()

        with jax.named_scope("solve_1"):
            solve(n, cx // 2, c1)

        @pl.when((n > 0) & has_right)
        def _():
            c1_copy(n, 0).start()

            @pl.when(n == nrhs - 1)
            def _():
                c1_copy(0, 1).start()

        return carry

    lax.fori_loop(0, nrhs, solve_1, 0)

    def look_1(n, row):
        img_rim(n).wait_send()
        with jax.named_scope("block"):
            upper, lower = block(n)

        @pl.when(has_left)
        def _():
            with jax.named_scope("c1_wait"):
                c1_copy(n, 0).wait_recv()

        with jax.named_scope("couple"):
            both = couple(n)
            row = row_of((sum(upper), sum(lower) - 2.0 * both), 2 * n, row)

            @pl.when(n == nrhs - 1)
            def _():
                share(second, row)

        @pl.when((n == nrhs - 1) & has_right)
        def _():
            for m in range(1, nrhs):
                c1_copy(m, 1).start()

        @pl.when(has_left)
        def _():
            c1_rim(n).start()

        cross(2, n).start()
        cross(3, n).start()
        return row

    blank = jnp.zeros((1, LANES), jnp.float32)
    lax.fori_loop(0, nrhs, look_1, blank)
    with jax.named_scope("total_1"):
        pick_second = totals(second)

    def finish_1(m, row):
        alpha = pick_second(2 * m) / pick_second(2 * m + 1)
        start = al[m]
        with jax.named_scope("cross_wait"):
            for k in range(3):
                cross_done(k, m, x_recv)

        def update(solution_planes, residual_planes):
            def body(j, carry):
                r = pl.multiple_of(own + j * ROWS, ROWS)
                here = pl.ds(r, ROWS)
                there = pl.ds(r + PAD, ROWS)
                step = pl.ds(pl.multiple_of(j * ROWS, ROWS), ROWS)
                near = pl.ds(pl.multiple_of(colour * own_rows + j * ROWS, ROWS), ROWS)
                far = pl.ds(pl.multiple_of((1 - colour) * own_rows + j * ROWS, ROWS), ROWS)
                for i in range(half):
                    t = colour * half + i
                    for p in solution_planes:
                        u = start * c0[m, p + 1, t, there, :]
                        sol[m, p, near, lane(i)] = u + alpha * c1[m, p + 1, t, there, :]
                        u = start * x_c0[m, p, i, step, :]
                        sol[m, p, far, lane(i)] = u + alpha * x_c1[m, p, i, step, :]
                    for p in residual_planes:
                        value = alpha * img[m, p, t, here, :]
                        res[m, p, near, lane(i)] = q[m, p + 1, t, here, :] - value
                        value = alpha * x_img[m, p, i, step, :]
                        res[m, p, far, lane(i)] = x_q[m, p, i, step, :] - value
                return carry

            lax.fori_loop(0, own_rows // ROWS, body, 0, unroll=2)

        with jax.named_scope("finish"):
            update(range(cx), range(1, cx))
            total = squares(m, alpha)

        @pl.when(has_left)
        def _():
            with jax.named_scope("edge_wait"):
                c1_rim(m).wait_recv()
                c1_copy(m, 1).wait_recv()

        with jax.named_scope("edge"):
            total = edge(m, alpha, total)
            cross(4, m).start()
            row = row_of((total,), m, row)

            @pl.when(m == nrhs - 1)
            def _():
                share(third, row)

            cross(4, m).wait_recv()
            update((), (0,))
        return row

    lax.fori_loop(0, nrhs, finish_1, blank)

    with jax.named_scope("norm"):
        arrived(slots.at[third, pl.ds(0, everyone - 1)], a_recv.at[third])
        found = jnp.sqrt(jnp.sum(slots[third], axis=0))
        norms[...] = found[0, 0:nrhs]

    with jax.named_scope("drain"):

        @pl.when(has_right)
        def _():
            arrived(dg.at[0, :, q_rows], q_send.at[nrhs])
            for n in range(nrhs):
                q1_rim(n).wait_send()
                c0_rim(n).wait_send()
                for k in range(2):
                    c1_copy(n, k).wait_send()

        @pl.when(has_left)
        def _():
            arrived(dg.at[cx + 1, :, q_rows], d_send)
            for n in range(nrhs):
                q_rim(n).wait_send()
                c1_rim(n).wait_send()
                c0_copy(n).wait_send()

        @pl.when(has_left & jnp.logical_not(has_right))
        def _():
            for n in range(nrhs):
                q_copy(n).wait_send()

        arrived(slots.at[:, pl.ds(0, everyone - 1)], a_send)
        for n in range(nrhs):
            for k in range(3):
                cross_done(k, n, x_send)
            cross(4, n).wait_send()


def store_kernel(sol_in, res_in, norms_in, sol, res, norms, sems):
    copies = []
    for n in range(sol.shape[0]):
        for src, dst in ((sol_in, sol), (res_in, res)):
            copies.append(pltpu.make_async_copy(src.at[n], dst.at[n], sems.at[len(copies)]))
    copies.append(pltpu.make_async_copy(norms_in, norms, sems.at[len(copies)]))
    for copy in copies:
        copy.start()
    for copy in copies:
        copy.wait()


def shards(rhs, diagonal):
    count = lax.axis_size("sub")
    nrhs, cx, ny, nz = rhs.shape
    assert cx == 4 and SWEEPS % 2 == 0
    tiles = nz // LANES
    rows = ny // 2 + RIM
    padded = rows + 2 * PAD
    f32 = jnp.float32
    out = jax.ShapeDtypeStruct((nrhs, cx, ny, nz // 2), f32)
    dma = pltpu.SemaphoreType.DMA
    crossed = pltpu.VMEM((nrhs, cx, tiles // 2, ny // 2, LANES), f32)
    remote = pl.BlockSpec(memory_space=pltpu.HBM)
    near = pl.BlockSpec(memory_space=pltpu.VMEM)
    sol, res, norms = pl.pallas_call(
        functools.partial(kernel, count),
        out_shape=(out, out, jax.ShapeDtypeStruct((nrhs,), f32)),
        in_specs=[remote, remote],
        out_specs=(near, near, near),
        scratch_shapes=[
            pltpu.VMEM((nrhs, cx + 2, tiles, rows, LANES), f32),
            pltpu.VMEM((nrhs, cx + 2, tiles, padded, LANES), f32),
            pltpu.VMEM((nrhs, cx + 2, tiles, padded, LANES), f32),
            pltpu.VMEM((nrhs, cx, tiles, rows, LANES), f32),
            pltpu.VMEM((cx + 2, tiles, rows, LANES), f32),
            pltpu.VMEM((cx + 2, tiles, rows, LANES), f32),
            pltpu.VMEM((2, cx // 2 + 2, tiles, padded, LANES), f32),
            pltpu.VMEM((nrhs, ROWS, LANES), f32),
            pltpu.VMEM((nrhs + 2, 2 * count, 1, LANES), f32),
            pltpu.VMEM((nrhs + 2, 1, LANES), f32),
            crossed, crossed, crossed, crossed,
            dma((nrhs + 1,)),
            dma((nrhs + 1,)), dma((nrhs + 1,)),
            dma, dma,
            dma((nrhs, 3)), dma((nrhs, 3)),
            dma((nrhs,)), dma((nrhs,)),
            dma((nrhs,)), dma((nrhs,)),
            dma, dma((nrhs + 2,)),
            dma((2 + 4 * nrhs,)), dma((2 + 4 * nrhs,)),
            dma((nrhs, 3)), dma((nrhs, 3)),
        ],
        compiler_params=pltpu.CompilerParams(
            collective_id=0, has_side_effects=True, vmem_limit_bytes=44 << 20
        ),
        name="schwarz",
    )(
        pltpu.with_memory_space_constraint(rhs, pltpu.HBM),
        pltpu.with_memory_space_constraint(diagonal, pltpu.HBM),
    )
    return pl.pallas_call(
        store_kernel,
        out_shape=(out, out, jax.ShapeDtypeStruct((nrhs,), f32)),
        in_specs=[pl.BlockSpec(memory_space=pl.ANY)] * 3,
        out_specs=(remote, remote, remote),
        scratch_shapes=[dma((2 * nrhs + 1,))],
        compiler_params=pltpu.CompilerParams(vmem_limit_bytes=1 << 20),
        name="store",
    )(sol, res, norms)


def solution(mesh):
    placed = (P(None, "sub", None, None), P("sub", None, None))
    return jax.shard_map(
        shards,
        mesh=mesh,
        in_specs=placed,
        out_specs=(P(None, "sub", None, "colour"), P(None, "sub", None, "colour"), P()),
        check_vma=False,
    )
```
